512 devices in a mesh: grp: 8 (over y), blk: 64 (over z, x, core).
Axes of the slice: x: 4, y: 8, z: 8, core: 2. Of those that a mesh axis runs over, the one named last changes fastest.
Arguments:
- query_rows: bfloat16 [12288, 4096], P('blk', 'grp'), may hold values from -128 to 128
- key_rows: bfloat16 [12288, 512], P(('grp', 'blk')), may hold values from -6 to 6
- value_rows: bfloat16 [12288, 512], P(('grp', 'blk')), may hold values from -6 to 6
- span_ids: int32 [128], P('blk'), may hold values from 0 to 127, as said below
Outputs:
- attended: bfloat16 [12288, 4096], P('blk', 'grp')
The draws below stay inside these ranges and needn't reach their ends.
Inputs may be any that keep to these rules, and one draw needn't show every extreme that they name: `span_ids`: A permutation of 0 to 127; each device of blk holds two entries, in device order.
All inputs are finite; a program needn't handle non-finite values.
Results may differ from the reference program's by a relative error of at most 0.0045.
Values may be sent and summed in bfloat16 or wider, within the bound.
No kernel may reach another device: no remote copies, remote signals or barrier semaphores. Data moves between devices by JAX's collectives and lax.ppermute only.
A program may use at most 64 MiB of HBM per device.

```python
import math
import jax
import jax.numpy as jnp
from jax import lax

HEADS = 32
KV_HEADS = 4
HEAD_DIM = 128
SPAN = 96
SEQ = 12288
SPANS = 128


def shared_keys(key):
    raw = jax.random.normal(jax.random.fold_in(key, 7), (SEQ, KV_HEADS, HEAD_DIM), jnp.float32)
    return jnp.clip(raw, -5.0, 5.0)


def draw_query_rows(key, part):
    base = jax.random.normal(jax.random.fold_in(key, 3), (SEQ, HEADS * HEAD_DIM), jnp.float32)
    base = 3.0 * jnp.clip(base, -6.0, 6.0)
    return base.astype(jnp.bfloat16)


def draw_key_rows(key, part):
    keys_out = shared_keys(key)
    return keys_out.reshape(SEQ, KV_HEADS * HEAD_DIM).astype(jnp.bfloat16)


def draw_span_ids(key, part):
    return jax.random.permutation(jax.random.fold_in(key, 11), SPANS).astype(jnp.int32)


def shard_levels(key, extent, cuts, least, high):
    def one(dim, parts):
        heights = jax.random.uniform(jax.random.fold_in(jax.random.fold_in(key, 6), dim), (parts,), jnp.float32, least / len(cuts), high / len(cuts))
        return jnp.repeat(jnp.exp(heights), extent[dim] // parts).reshape((-1,) + (1,) * (len(extent) - dim - 1))

    factor_of = one(*cuts[0])
    for cut in cuts[1:]:
        factor_of = factor_of * one(*cut)
    return factor_of


def normal_values(key, shape, spread, limit, pieces=(), held_as=jnp.bfloat16):
    entries = jax.random.normal(key, shape, jnp.float32) * spread
    if len(pieces) > 0:
        entries = shard_levels(key, shape, pieces, -0.22, 0.18) * entries
    return jnp.clip(entries, min=-limit, max=limit).astype(held_as)


def setup_inputs(seed: int = 0) -> dict:
    streams_of = jax.random.split(jax.random.key(seed), 5)
    query_rows = draw_query_rows(jax.random.fold_in(streams_of[4], 71), 0)
    key_rows = draw_key_rows(jax.random.fold_in(streams_of[4], 71), 0)
    value_rows = normal_values(streams_of[2], (SEQ, KV_HEADS * HEAD_DIM), 1.0, 6.0, ((0, 512),))
    span_ids = draw_span_ids(jax.random.fold_in(streams_of[4], 71), 0)
    return dict(query_rows=query_rows, key_rows=key_rows, value_rows=value_rows, span_ids=span_ids)


def reference(query_rows, key_rows, value_rows, span_ids):
    rows = jnp.arange(SEQ, dtype=jnp.int32)
    positions = (span_ids[rows // SPAN] * SPAN + rows % SPAN).astype(jnp.int32)
    ratio = HEADS // KV_HEADS
    scale = HEAD_DIM ** -0.5
    keys_all = key_rows.reshape(SEQ, KV_HEADS, HEAD_DIM).astype(jnp.float32)
    values_all = value_rows.reshape(SEQ, KV_HEADS, HEAD_DIM).astype(jnp.float32)
    block_rows = math.gcd(SEQ, 256)

    def one_block(start):
        query_block = lax.dynamic_slice_in_dim(query_rows, start, block_rows, 0)
        query_block = query_block.reshape(block_rows, KV_HEADS, ratio, HEAD_DIM).astype(jnp.float32)
        query_pos = lax.dynamic_slice_in_dim(positions, start, block_rows, 0)
        scores = jnp.einsum('tgrd,ngd->grtn', query_block, keys_all) * scale
        allowed = positions[None, :] <= query_pos[:, None]
        scores = jnp.where(allowed, scores, -jnp.inf)
        top = jnp.max(scores, axis=-1, keepdims=True)
        weights = jnp.where(allowed, jnp.exp(scores - top), 0.0).astype(jnp.bfloat16)
        weights_wide = weights.astype(jnp.float32)
        total = jnp.sum(weights_wide, axis=-1)
        mixed = jnp.einsum('grtn,ngd->grtd', weights_wide, values_all) / total[..., None]
        mixed = jnp.transpose(mixed, (2, 0, 1, 3)).reshape(block_rows, HEADS * HEAD_DIM)
        return mixed.astype(jnp.bfloat16)

    starts = (jnp.arange(SEQ // block_rows) * block_rows).astype(jnp.int32)
    blocks_out = lax.map(one_block, starts)
    return blocks_out.reshape(SEQ, HEADS * HEAD_DIM)
```

```python
import functools
import math

import jax
import jax.numpy as jnp
from jax import lax
from jax.experimental import pallas as pl
from jax.experimental.pallas import tpu as pltpu
from jax.sharding import Mesh
from jax.sharding import PartitionSpec as P


HEAD_DIM = 128
SPAN = 96
PIECE = 24
ROWS = 208
HEADS = 4
COLS = 2 * HEADS * SPAN
STATE = 144
TILE = 256
MASKED = -1e30
FACTOR = HEAD_DIM**-0.5 * math.log2(math.e)
AXES = ("kv", "pair", "z", "x", "core")
BLK = ("z", "x", "core")
F32 = jnp.float32
BF16 = jnp.bfloat16


def pack_kernel(key_ref, value_ref, ids_ref, out_ref):
    out_ref[:, 48:56, :] = jnp.broadcast_to(ids_ref[...][None], (4, 8, HEAD_DIM))
    for head in range(4):
        lanes = slice(head * HEAD_DIM, (head + 1) * HEAD_DIM)
        out_ref[head, 0:24, :] = key_ref[:, lanes]
        out_ref[head, 24:48, :] = value_ref[:, lanes]


def spread_kernel(routed_ref, out_ref):
    routed = routed_ref[...].astype(F32)
    parts = [routed[s, 0:24] for s in range(4)] + [routed[s, 24:48] for s in range(4)]
    parts += [routed[s, 48:56] for s in range(4)]
    ids = jnp.concatenate([routed[s, 48:52] for s in range(4)], axis=0)
    block = jnp.concatenate(parts[:8] + [ids], axis=0).astype(BF16)
    for z in range(8):
        out_ref[z] = block


def attend_kernel(count, offsets, own_core, has_state, last, *refs):
    refs = list(refs)
    q_refs = [refs.pop(0), refs.pop(0)]
    blocks = [refs.pop(0) for _ in range(count)]
    table_src = blocks[0] if offsets[0] == 0 else refs.pop(0)
    state_ref = refs.pop(0) if has_state else None
    out_ref, table, turned = refs

    x = lax.axis_index("x")
    core = lax.axis_index("core")
    pair = lax.axis_index("pair")
    z_here = lax.axis_index("z")
    span = pl.program_id(0)
    keys = 768 * count

    @pl.when(span == 0)
    def _():
        for z in range(8):
            table[z * 16 : (z + 1) * 16, :] = table_src[z, 192:208, :].astype(F32)
        turned[128:144, :] = jnp.ones((16, keys), BF16)
        for b in range(count):
            values = jnp.concatenate([blocks[b][z, 96:192, :] for z in range(8)], axis=0)
            turned[0:128, b * 768 : (b + 1) * 768] = values.T

    query_row = table[pl.ds(z_here * 16 + (0 if own_core else 2) + span, 1), :]
    lane = lax.broadcasted_iota(jnp.int32, (PIECE, HEAD_DIM), 1)
    row = lax.broadcasted_iota(jnp.int32, (PIECE, HEAD_DIM), 0)
    ahead = (row - lane).astype(F32)

    wide = []
    for b in range(count):
        from_x = lax.rem(x + (4 + offsets[b]), 4)
        entry = from_x // 2
        first = ((lax.rem(from_x, 2) * 2 + core) * PIECE).astype(F32)
        for z in range(8):
            pieces = []
            for s in range(4):
                index = (
                    (2 * s + pair) * 16
                    + lax.rem(x + (4 - z // 2), 4) * 4
                    + (core if z % 2 == 0 else 1 - core) * 2
                    + entry
                )
                key_row = table[pl.ds(index, 1), :]
                limit = (query_row - key_row) * float(SPAN) - first
                pieces.append(
                    jnp.where(ahead > jnp.broadcast_to(limit, ahead.shape), MASKED, 0.0)
                )
            mask = jnp.concatenate(pieces, axis=0).astype(BF16)
            wide.append(jnp.concatenate([blocks[b][z, 0:96, :], mask], axis=1))
    wide = jnp.concatenate(wide, axis=0)

    spot = lax.broadcasted_iota(jnp.int32, (SPAN, HEAD_DIM), 0)
    mark = lax.broadcasted_iota(jnp.int32, (SPAN, HEAD_DIM), 1)
    one_hot = jnp.where(spot == mark, 1.0, 0.0).astype(BF16)
    queries = [
        jnp.concatenate([q[..., h * HEAD_DIM : (h + 1) * HEAD_DIM].reshape(SPAN, HEAD_DIM), one_hot], axis=1)
        for q in q_refs
        for h in range(HEADS)
    ]
    queries = jnp.concatenate(queries, axis=0)

    flip = (((1,), (1,)), ((), ()))
    for t in range(COLS // TILE):
        cols = slice(t * TILE, (t + 1) * TILE)
        scores = lax.dot_general(wide, queries[cols], flip, preferred_element_type=F32)
        top = jnp.max(scores, axis=0, keepdims=True)
        if has_state:
            before = state_ref[0, 136:137, cols]
            top = jnp.maximum(before, top)
        weights = jnp.exp2((scores - top) * FACTOR).astype(BF16)
        sums = jnp.dot(turned[...], weights, preferred_element_type=F32)[0:136]
        if has_state:
            sums = sums + state_ref[0, 0:136, cols] * jnp.exp2((before - top) * FACTOR)
        if last:
            pack_state(out_ref, (0,), cols, sums[0:128], sums[128:129], top)
        else:
            out_ref[0, 0:136, cols] = sums
            out_ref[0, 136:144, cols] = jnp.broadcast_to(top, (8, TILE))


def pack_state(out_ref, lead, cols, weighted, total, top):
    out_ref[(*lead, slice(0, 128), cols)] = weighted.astype(BF16)
    width = top.shape[1]
    line = lax.broadcasted_iota(jnp.int32, (16, width), 0)
    stats = jnp.zeros((16, width), F32)
    for base, value in ((0, top), (3, total)):
        for k in range(3):
            part = value.astype(BF16).astype(F32)
            value = value - part
            stats = jnp.where(line == base + k, jnp.broadcast_to(part, stats.shape), stats)
    out_ref[(*lead, slice(128, 144), cols)] = stats.astype(BF16)


def open_state(ref, lead, cols):
    stats = ref[(*lead, slice(128, 144), cols)].astype(F32)
    top = stats[0:1] + stats[1:2] + stats[2:3]
    total = stats[3:4] + stats[4:5] + stats[5:6]
    return ref[(*lead, slice(0, 128), cols)].astype(F32), total, top


def merge(mine, other):
    top = jnp.maximum(mine[2], other[2])
    a = jnp.exp2((mine[2] - top) * FACTOR)
    b = jnp.exp2((other[2] - top) * FACTOR)
    return mine[0] * a + other[0] * b, mine[1] * a + other[1] * b, top


def join_kernel(state_ref, come_ref, own_ref, out_ref):
    half = COLS // 2
    for e in range(2):
        for side in range(2):
            cols = slice(side * half, (side + 1) * half)
            mine = (state_ref[e, 0:128, cols], state_ref[e, 128:129, cols], state_ref[e, 136:137, cols])
            weighted, total, top = merge(mine, open_state(come_ref, (e,), cols))
            if side == 0:
                own_ref[e, 0:128, :] = weighted
                own_ref[e, 128:136, :] = jnp.broadcast_to(total, (8, half))
                own_ref[e, 136:144, :] = jnp.broadcast_to(top, (8, half))
            else:
                pack_state(out_ref, (e,), slice(0, half), weighted, total, top)


def finish_kernel(own_ref, come_ref, out_ref):
    half = COLS // 2
    everything = slice(0, half)
    for e in range(2):
        mine = (own_ref[e, 0:128, :], own_ref[e, 128:129, :], own_ref[e, 136:137, :])
        weighted, total, _ = merge(mine, open_state(come_ref, (e,), everything))
        mixed = (weighted / total).T.astype(BF16)
        for h in range(HEADS):
            out_ref[e * SPAN : (e + 1) * SPAN, h * HEAD_DIM : (h + 1) * HEAD_DIM] = mixed[
                h * SPAN : (h + 1) * SPAN
            ]


def whole(shape):
    return pl.BlockSpec(shape, lambda e: (0,) * len(shape))


def attend(q_args, q_specs, blocks, offsets, table_src, state, own_core, last):
    count = len(blocks)
    kernel = functools.partial(
        attend_kernel, count, offsets, own_core, state is not None, last
    )
    block_spec = whole((8, ROWS, HEAD_DIM))
    args = [*q_args, *blocks]
    specs = [*q_specs, *([block_spec] * count)]
    if offsets[0] != 0:
        args.append(table_src)
        specs.append(block_spec)
    state_spec = pl.BlockSpec((1, STATE, COLS), lambda e: (e, 0, 0))
    if state is not None:
        args.append(state)
        specs.append(state_spec)
    macs = 2 * COLS * 768 * count * (256 + STATE)
    return pl.pallas_call(
        kernel,
        grid=(2,),
        in_specs=specs,
        out_specs=state_spec,
        out_shape=jax.ShapeDtypeStruct((2, STATE, COLS), BF16 if last else F32),
        scratch_shapes=[
            pltpu.VMEM((128, HEAD_DIM), F32),
            pltpu.VMEM((STATE, 768 * count), BF16),
        ],
        compiler_params=pltpu.CompilerParams(
            dimension_semantics=("arbitrary",), vmem_limit_bytes=48 * 1024 * 1024
        ),
        cost_estimate=pl.CostEstimate(
            flops=2 * macs, bytes_accessed=2**20, transcendentals=2 * COLS * 768 * count
        ),
        name=f"attend_{'own' if own_core else 'other'}_{count}_{offsets[0] % 4}",
    )(*args)


def call(kernel, out_shape, *args):
    return pl.pallas_call(
        kernel,
        out_shape=out_shape,
        compiler_params=pltpu.CompilerParams(vmem_limit_bytes=16 * 1024 * 1024),
        cost_estimate=pl.CostEstimate(flops=2**21, bytes_accessed=2**20, transcendentals=0),
    )(*args)


def shifted(value, axis, step):
    size = lax.axis_size(axis)
    return lax.ppermute(value, axis, [(i, (i + step) % size) for i in range(size)])


def spread_ids(ids, swap):
    kv, xs, cores = lax.axis_size("kv"), lax.axis_size("x"), lax.axis_size("core")
    perm = []
    for k in range(kv):
        for x in range(xs):
            for c in range(cores):
                to = (k * xs + (x + k) % xs) * cores + (c ^ swap)
                perm.append(((k * xs + x) * cores + c, to))
    return lax.ppermute(ids, ("kv", "x", "core"), perm)


def body(query_rows, key_rows, value_rows, span_ids):
    ids = jnp.broadcast_to(span_ids.astype(F32)[:, None], (2, HEAD_DIM)).astype(BF16)
    seen = jnp.concatenate(
        [spread_ids(ids, 0), spread_ids(ids, 1), jnp.zeros((4, HEAD_DIM), BF16)], axis=0
    )
    packed = call(
        pack_kernel, jax.ShapeDtypeStruct((4, 56, HEAD_DIM), BF16), key_rows, value_rows, seen
    )
    routed = lax.all_to_all(packed, "kv", 0, 0, tiled=True)
    copies = call(spread_kernel, jax.ShapeDtypeStruct((8, ROWS, HEAD_DIM), BF16), routed)
    near = lax.all_to_all(copies, "z", 0, 0, tiled=True)

    beyond = shifted(query_rows, "pair", 1)
    right, left, far = (shifted(near, "x", d) for d in (-1, 1, 2))
    across = shifted(jnp.stack([query_rows, beyond]), "core", 1)

    half = (SPAN, HEADS * HEAD_DIM)
    own_q = ((query_rows, beyond), [pl.BlockSpec(half, lambda e: (e, 0))] * 2)
    other_q = (
        (across, across),
        [
            pl.BlockSpec((1, *half), lambda e: (0, e, 0)),
            pl.BlockSpec((1, *half), lambda e: (1, e, 0)),
        ],
    )

    states = {}
    for own, q in ((True, own_q), (False, other_q)):
        state = attend(*q, [near], [0], None, None, own, False)
        state = attend(*q, [right, left], [1, 3], near, state, own, False)
        states[own] = (q, state)
    q, state = states[False]
    leaving = attend(*q, [far], [2], near, state, False, True)
    q, state = states[True]
    coming = shifted(leaving, "core", 1)
    mine = attend(*q, [far], [2], near, state, True, False)
    own, leaving = call(
        join_kernel,
        (
            jax.ShapeDtypeStruct((2, STATE, COLS // 2), F32),
            jax.ShapeDtypeStruct((2, STATE, COLS // 2), BF16),
        ),
        mine,
        coming,
    )
    coming = shifted(leaving, "pair", 1)
    return call(
        finish_kernel, jax.ShapeDtypeStruct((2 * SPAN, HEADS * HEAD_DIM), BF16), own, coming
    )


def solution(mesh):
    split = Mesh(mesh.devices.reshape(4, 2, 8, 4, 2), AXES)
    groups = ("kv", "pair")
    return jax.shard_map(
        body,
        mesh=split,
        in_specs=(P(BLK, groups), P(groups + BLK, None), P(groups + BLK, None), P(BLK)),
        out_specs=P(BLK, groups),
        check_vma=False,
    )
```

```python
import functools
import math

import jax
import jax.numpy as jnp
from jax import lax
from jax.experimental import pallas as pl
from jax.experimental.pallas import tpu as pltpu
from jax.sharding import Mesh
from jax.sharding import PartitionSpec as P


HEAD_DIM = 128
SPAN = 96
PIECE = 24
ROWS = 200
HEADS = 4
COLS = 2 * HEADS * SPAN
STATE = 144
TILE = 256
CHUNK = 768
MASKED = -1e30
FACTOR = HEAD_DIM**-0.5 * math.log2(math.e)
AXES = ("kv", "pair", "z", "x", "core")
BLK = ("z", "x", "core")
F32 = jnp.float32
BF16 = jnp.bfloat16


def pack_kernel(key_ref, value_ref, ids_ref, out_ref):
    second = lax.axis_index("x") // 2 == 1
    own = jnp.where(second, ids_ref[1:2, :], ids_ref[0:1, :])
    own = jnp.broadcast_to(own, (8, HEAD_DIM)).astype(BF16)
    for head in range(4):
        lanes = slice(head * HEAD_DIM, (head + 1) * HEAD_DIM)
        out_ref[head, 0:24, :] = key_ref[:, lanes]
        out_ref[head, 24:48, :] = value_ref[:, lanes]
        out_ref[head, 48:56, :] = own


def spread_kernel(routed_ref, out_ref):
    routed = routed_ref[...].astype(F32)
    parts = [routed[s, 0:24] for s in range(4)] + [routed[s, 24:48] for s in range(4)]
    ids = [routed[s, 48:49] for s in range(4)]
    block = jnp.concatenate(parts + ids + ids, axis=0).astype(BF16)
    for z in range(8):
        out_ref[z] = block


def stack_kernel(own_ref, beyond_ref, ids_ref, out_ref):
    out_ref[0, 0:192, :] = own_ref[...]
    out_ref[1, 0:192, :] = beyond_ref[...]
    ids = jnp.concatenate([ids_ref[...]] * HEADS, axis=1)
    ids = jnp.concatenate([ids] * 4, axis=0).astype(BF16)
    out_ref[0, 192:200, :] = ids
    out_ref[1, 192:200, :] = ids


def attend_kernel(count, offsets, sets, has_state, last, *refs):
    refs = list(refs)
    q_refs = {s: [refs.pop(0), refs.pop(0), refs.pop(0)] for s in sets}
    blocks = [refs.pop(0) for _ in range(count)]
    state_ref = refs.pop(0) if has_state else None
    out_ref, ids, turned, wide, queries, held, weights = refs

    x = lax.axis_index("x")
    core = lax.axis_index("core")
    step = pl.program_id(0)
    keys = 768 * count

    @pl.when(step == 0)
    def _():
        turned[128:144, :] = jnp.ones((16, keys), BF16)
        for b in range(count):
            values = jnp.concatenate([blocks[b][z, 96:192, :] for z in range(8)], axis=0)
            turned[0:128, b * 768 : (b + 1) * 768] = values.T
            for z in range(8):
                at = b * 768 + z * SPAN
                wide[at : at + SPAN, 0:128] = blocks[b][z, 0:96, :]
        spot = lax.broadcasted_iota(jnp.int32, (SPAN, HEAD_DIM), 0)
        mark = lax.broadcasted_iota(jnp.int32, (SPAN, HEAD_DIM), 1)
        one_hot = jnp.where(spot == mark, 1.0, 0.0).astype(BF16)
        for k in range(2 * HEADS):
            queries[k * SPAN : (k + 1) * SPAN, 128:256] = one_hot

    def fetch(s):
        mine, beyond, places = q_refs[s]
        for k in range(2 * HEADS):
            h = k % HEADS
            source = mine if k < HEADS else beyond
            piece = source[0, :, h * HEAD_DIM : (h + 1) * HEAD_DIM]
            queries[k * SPAN : (k + 1) * SPAN, 0:128] = piece
        places = places[0, :, 0:HEAD_DIM].astype(F32)
        ids[...] = jnp.where(lax.rem(step, 2) == 0, places[0:1], places[1:2])

    if len(sets) == 1:
        fetch(sets[0])
    else:
        for i, s in enumerate(sets):
            pl.when(step // 2 == i)(functools.partial(fetch, s))

    query_row = ids[...]
    lane = lax.broadcasted_iota(jnp.int32, (PIECE, HEAD_DIM), 1)
    row = lax.broadcasted_iota(jnp.int32, (PIECE, HEAD_DIM), 0)
    ahead = (row - lane).astype(F32)
    for b in range(count):
        from_x = lax.rem(x + (4 + offsets[b]), 4)
        first = ((lax.rem(from_x, 2) * 2 + core) * PIECE).astype(F32)
        for z in range(8):
            places = blocks[b][z, 192:200, :].astype(F32)
            pieces = []
            for s in range(4):
                limit = (query_row - places[s : s + 1]) * float(SPAN) - first
                pieces.append(
                    jnp.where(ahead > jnp.broadcast_to(limit, ahead.shape), MASKED, 0.0)
                )
            at = b * 768 + z * SPAN
            wide[at : at + SPAN, 128:256] = jnp.concatenate(pieces, axis=0).astype(BF16)

    flip = (((1,), (1,)), ((), ()))

    def score(t):
        best = None
        for c in range(keys // CHUNK):
            rows = slice(c * CHUNK, (c + 1) * CHUNK)
            part = lax.dot_general(
                wide[rows, :],
                queries[t * TILE : (t + 1) * TILE, :],
                flip,
                preferred_element_type=F32,
            )
            held[t % 2, rows, :] = part
            peak = jnp.max(part.reshape(CHUNK // 8, 8, TILE), axis=0)
            best = peak if best is None else jnp.maximum(best, peak)
        return best

    tiles = COLS // TILE
    best = score(0)
    for t in range(tiles):
        cols = slice(t * TILE, (t + 1) * TILE)
        top = jnp.max(best, axis=0, keepdims=True)
        if t + 1 < tiles:
            best = score(t + 1)
        if has_state:
            before = state_ref[0, 136:137, cols]
            top = jnp.maximum(before, top)
        for c in range(keys // CHUNK):
            rows = slice(c * CHUNK, (c + 1) * CHUNK)
            weights[t % 2, rows, :] = jnp.exp2((held[t % 2, rows, :] - top) * FACTOR).astype(BF16)
        sums = jnp.dot(turned[...], weights[t % 2], preferred_element_type=F32)[0:136]
        if has_state:
            sums = sums + state_ref[0, 0:136, cols] * jnp.exp2((before - top) * FACTOR)
        if last:
            pack_state(out_ref, (0,), cols, sums[0:128], sums[128:129], top)
        else:
            out_ref[0, 0:136, cols] = sums
            out_ref[0, 136:144, cols] = jnp.broadcast_to(top, (8, TILE))


def pack_state(out_ref, lead, cols, weighted, total, top):
    out_ref[(*lead, slice(0, 128), cols)] = weighted.astype(BF16)
    width = top.shape[1]
    line = lax.broadcasted_iota(jnp.int32, (16, width), 0)
    stats = jnp.zeros((16, width), F32)
    for base, value in ((0, top), (3, total)):
        for k in range(3):
            part = value.astype(BF16).astype(F32)
            value = value - part
            stats = jnp.where(line == base + k, jnp.broadcast_to(part, stats.shape), stats)
    out_ref[(*lead, slice(128, 144), cols)] = stats.astype(BF16)


def open_state(ref, lead, cols):
    stats = ref[(*lead, slice(128, 144), cols)].astype(F32)
    top = stats[0:1] + stats[1:2] + stats[2:3]
    total = stats[3:4] + stats[4:5] + stats[5:6]
    return ref[(*lead, slice(0, 128), cols)].astype(F32), total, top


def merge(mine, other):
    top = jnp.maximum(mine[2], other[2])
    a = jnp.exp2((mine[2] - top) * FACTOR)
    b = jnp.exp2((other[2] - top) * FACTOR)
    return mine[0] * a + other[0] * b, mine[1] * a + other[1] * b, top


def join_kernel(state_ref, come_ref, own_ref, out_ref):
    half = COLS // 2
    for e in range(2):
        for side in range(2):
            cols = slice(side * half, (side + 1) * half)
            mine = (state_ref[e, 0:128, cols], state_ref[e, 128:129, cols], state_ref[e, 136:137, cols])
            weighted, total, top = merge(mine, open_state(come_ref, (e,), cols))
            if side == 0:
                own_ref[e, 0:128, :] = weighted
                own_ref[e, 128:136, :] = jnp.broadcast_to(total, (8, half))
                own_ref[e, 136:144, :] = jnp.broadcast_to(top, (8, half))
            else:
                pack_state(out_ref, (e,), slice(0, half), weighted, total, top)


def finish_kernel(own_ref, come_ref, out_ref):
    half = COLS // 2
    everything = slice(0, half)
    for e in range(2):
        mine = (own_ref[e, 0:128, :], own_ref[e, 128:129, :], own_ref[e, 136:137, :])
        weighted, total, _ = merge(mine, open_state(come_ref, (e,), everything))
        mixed = (weighted / total).T.astype(BF16)
        for h in range(HEADS):
            out_ref[e * SPAN : (e + 1) * SPAN, h * HEAD_DIM : (h + 1) * HEAD_DIM] = mixed[
                h * SPAN : (h + 1) * SPAN
            ]


def whole(shape):
    return pl.BlockSpec(shape, lambda e: (0,) * len(shape))


def attend(stacks, sets, blocks, offsets, state, last):
    count = len(blocks)
    steps = 2 * len(sets)
    kernel = functools.partial(attend_kernel, count, offsets, sets, state is not None, last)
    args, specs = [], []
    for i, s in enumerate(sets):
        lane = HEADS * HEAD_DIM
        for plane in range(2):
            args.append(stacks[s])
            specs.append(
                pl.BlockSpec(
                    (1, SPAN, lane),
                    lambda e, i=i, plane=plane: (plane, jnp.clip(e - 2 * i, 0, 1), 0),
                )
            )
        args.append(stacks[s])
        specs.append(pl.BlockSpec((1, 8, lane), lambda e: (0, 24, 0)))
    args += blocks
    specs += [whole((8, ROWS, HEAD_DIM))] * count
    if state is not None:
        base = 2 * sets[0]
        args.append(state)
        specs.append(pl.BlockSpec((1, STATE, COLS), lambda e: (e + base, 0, 0)))
    macs = steps * COLS * 768 * count * (256 + STATE)
    return pl.pallas_call(
        kernel,
        grid=(steps,),
        in_specs=specs,
        out_specs=pl.BlockSpec((1, STATE, COLS), lambda e: (e, 0, 0)),
        out_shape=jax.ShapeDtypeStruct((steps, STATE, COLS), BF16 if last else F32),
        scratch_shapes=[
            pltpu.VMEM((1, HEAD_DIM), F32),
            pltpu.VMEM((STATE, 768 * count), BF16),
            pltpu.VMEM((768 * count, 256), BF16),
            pltpu.VMEM((COLS, 256), BF16),
            pltpu.VMEM((2, 768 * count, TILE), F32),
            pltpu.VMEM((2, 768 * count, TILE), BF16),
        ],
        compiler_params=pltpu.CompilerParams(
            dimension_semantics=("arbitrary",), vmem_limit_bytes=40 * 1024 * 1024
        ),
        cost_estimate=pl.CostEstimate(
            flops=4 * macs, bytes_accessed=2**20, transcendentals=steps * COLS * 768 * count
        ),
        name=f"attend_{len(sets)}_{sets[0]}_{count}_{offsets[0]}",
    )(*args)


def call(kernel, out_shape, *args):
    return pl.pallas_call(
        kernel,
        out_shape=out_shape,
        compiler_params=pltpu.CompilerParams(vmem_limit_bytes=16 * 1024 * 1024),
        cost_estimate=pl.CostEstimate(flops=2**21, bytes_accessed=2**20, transcendentals=0),
    )(*args)


def shifted(value, axis, step):
    size = lax.axis_size(axis)
    return lax.ppermute(value, axis, [(i, (i + step) % size) for i in range(size)])


def ids_to_keys(ids):
    size = {a: lax.axis_size(a) for a in AXES}

    def flat(kv, pair, z, x, core):
        return (((kv * size["pair"] + pair) * size["z"] + z) * size["x"] + x) * size["core"] + core

    perm = []
    for g in range(8):
        for z in range(8):
            for x in range(4):
                for c in range(2):
                    to = flat(z // 2, z % 2, x * 2 + c, g // 2, g % 2)
                    perm.append((flat(g // 2, g % 2, z, x, c), to))
    return lax.ppermute(ids, AXES, perm)


def body(query_rows, key_rows, value_rows, span_ids):
    ids = jnp.broadcast_to(span_ids.astype(F32)[:, None], (2, HEAD_DIM))
    packed = call(
        pack_kernel,
        jax.ShapeDtypeStruct((4, 56, HEAD_DIM), BF16),
        key_rows,
        value_rows,
        ids_to_keys(ids),
    )
    routed = lax.all_to_all(packed, "kv", 0, 0, tiled=True)
    copies = call(spread_kernel, jax.ShapeDtypeStruct((8, ROWS, HEAD_DIM), BF16), routed)
    near = lax.all_to_all(copies, "z", 0, 0, tiled=True)

    beyond = shifted(query_rows, "pair", 1)
    right, left = shifted(near, "x", -1), shifted(near, "x", 1)
    stack = call(
        stack_kernel,
        jax.ShapeDtypeStruct((2, 200, HEADS * HEAD_DIM), BF16),
        query_rows,
        beyond,
        ids,
    )
    stacks = (stack, shifted(stack, "core", 1))
    again, right, left = lax.optimization_barrier((near, right, left))
    far = shifted(again, "x", 2)

    state = attend(stacks, (0, 1), [near], [0], None, False)
    state = attend(stacks, (0, 1), [right, left], [1, 3], state, False)
    leaving = attend(stacks, (1,), [far], [2], state, True)
    coming = shifted(leaving, "core", 1)
    mine = attend(stacks, (0,), [far], [2], state, False)
    own, leaving = call(
        join_kernel,
        (
            jax.ShapeDtypeStruct((2, STATE, COLS // 2), F32),
            jax.ShapeDtypeStruct((2, STATE, COLS // 2), BF16),
        ),
        mine,
        coming,
    )
    coming = shifted(leaving, "pair", 1)
    return call(
        finish_kernel, jax.ShapeDtypeStruct((2 * SPAN, HEADS * HEAD_DIM), BF16), own, coming
    )


def solution(mesh):
    split = Mesh(mesh.devices.reshape(4, 2, 8, 4, 2), AXES)
    groups = ("kv", "pair")
    return jax.shard_map(
        body,
        mesh=split,
        in_specs=(P(BLK, groups), P(groups + BLK, None), P(groups + BLK, None), P(BLK)),
        out_specs=P(BLK, groups),
        check_vma=False,
    )
```

```python
import functools
import math

import jax
import jax.numpy as jnp
from jax import lax
from jax.experimental import pallas as pl
from jax.experimental.pallas import tpu as pltpu
from jax.sharding import Mesh
from jax.sharding import PartitionSpec as P


HEAD_DIM = 128
SPAN = 96
PIECE = 24
ROWS = 784
KEYS = 384
HEADS = 4
COLS = 2 * HEADS * SPAN
STATE = 144
TILE = 256
CHUNK = 128
MASKED = -1e30
FACTOR = HEAD_DIM**-0.5 * math.log2(math.e)
AXES = ("kv", "pair", "z", "x", "core")
BLK = ("z", "x", "core")
F32 = jnp.float32
BF16 = jnp.bfloat16


def pack_kernel(key_ref, value_ref, ids_ref, out_ref):
    own = jnp.concatenate([ids_ref[...]] * 4, axis=0).astype(BF16)
    for head in range(4):
        lanes = slice(head * HEAD_DIM, (head + 1) * HEAD_DIM)
        for x in range(4):
            out_ref[head, x, 0:24, :] = key_ref[:, lanes]
            out_ref[head, x, 24:48, :] = value_ref[:, lanes]
            out_ref[head, x, 48:56, :] = own


def spread_kernel(routed_ref, out_ref):
    for k in range(4):
        for x in range(4):
            at = (k * 4 + x) * PIECE
            out_ref[at : at + PIECE, :] = routed_ref[k, x, 0:24, :]
            out_ref[KEYS + at : KEYS + at + PIECE, :] = routed_ref[k, x, 24:48, :]
    rows = []
    for k in range(4):
        ids = sum(routed_ref[k, x, 48:56, :].astype(F32) for x in range(4))
        rows += [ids[0:1], ids[0:1], ids[1:2], ids[1:2]]
    out_ref[2 * KEYS : ROWS, :] = jnp.concatenate(rows, axis=0).astype(BF16)


def stack_kernel(own_ref, beyond_ref, ids_ref, out_ref):
    ids = jnp.concatenate([ids_ref[...]] * 8, axis=0).astype(BF16)
    for e in range(2):
        for k in range(2 * HEADS):
            h = k % HEADS
            source = own_ref if k < HEADS else beyond_ref
            out_ref[e, k * SPAN : (k + 1) * SPAN, :] = source[
                e * SPAN : (e + 1) * SPAN, h * HEAD_DIM : (h + 1) * HEAD_DIM
            ]
        out_ref[e, COLS : COLS + 16, :] = ids


def attend_kernel(count, sets, has_state, last, *refs):
    refs = list(refs)
    q_refs = [refs.pop(0) for _ in sets]
    blocks = [refs.pop(0) for _ in range(count)]
    state_ref = refs.pop(0) if has_state else None
    out_ref, turned, masks, one_hot, *held = refs
    weights, held = held[2:], held[:2]
    core = lax.axis_index("core")
    keys = KEYS * count

    turned[128:144, :] = jnp.ones((16, keys), BF16)
    for b in range(count):
        turned[0:128, b * KEYS : (b + 1) * KEYS] = blocks[b][KEYS : 2 * KEYS, :].T
    spot = lax.broadcasted_iota(jnp.int32, (SPAN, HEAD_DIM), 0)
    mark = lax.broadcasted_iota(jnp.int32, (SPAN, HEAD_DIM), 1)
    spike = jnp.where(spot == mark, 1.0, 0.0).astype(BF16)
    for k in range(2 * HEADS):
        one_hot[k * SPAN : (k + 1) * SPAN, :] = spike

    lane = lax.broadcasted_iota(jnp.int32, (PIECE, HEAD_DIM), 1)
    row = lax.broadcasted_iota(jnp.int32, (PIECE, HEAD_DIM), 0)
    begin = (core * PIECE).astype(F32)
    ahead = (row - lane).astype(F32) + begin

    def mask(s):
        query_row = q_refs[s // 2][s % 2, COLS : COLS + 16, :].astype(F32)[s % 2 : s % 2 + 1]
        for b in range(count):
            places = blocks[b][2 * KEYS : ROWS, :].astype(F32)
            limits = (query_row - places) * float(SPAN)
            for i in range(0, 16, 2):
                pieces = [
                    jnp.where(
                        ahead + float((j % 2) * 2 * PIECE)
                        > jnp.broadcast_to(limits[j : j + 1], ahead.shape),
                        MASKED,
                        0.0,
                    )
                    for j in (i, i + 1)
                ]
                at = b * KEYS + i * PIECE
                masks[s, at : at + 2 * PIECE, :] = jnp.concatenate(pieces, axis=0).astype(BF16)

    flip = (((1,), (1,)), ((), ()))
    tiles = [(s, t) for s in range(2 * len(sets)) for t in range(COLS // TILE)]

    def score(i):
        s, t = tiles[i]
        if t == 0:
            mask(s)
        cols = slice(t * TILE, (t + 1) * TILE)
        left = jnp.concatenate([blocks[b][0:KEYS, :] for b in range(count)], axis=0)
        left = jnp.concatenate([left, masks[s]], axis=1)
        right = jnp.concatenate([q_refs[s // 2][s % 2, cols, :], one_hot[cols, :]], axis=1)
        part = lax.dot_general(left, right, flip, preferred_element_type=F32)
        held[i % 2][...] = part
        return jnp.max(part.reshape(keys // 8, 8, TILE), axis=0)

    best = score(0)
    for i, (s, t) in enumerate(tiles):
        cols = slice(t * TILE, (t + 1) * TILE)
        top = jnp.max(best, axis=0, keepdims=True)
        if i + 1 < len(tiles):
            best = score(i + 1)
        if has_state:
            at = 2 * sets[0] + s
            before = state_ref[at, 136:137, cols]
            top = jnp.maximum(before, top)
        for c in range(keys // CHUNK):
            rows = slice(c * CHUNK, (c + 1) * CHUNK)
            weights[i % 2][rows, :] = jnp.exp2((held[i % 2][rows, :] - top) * FACTOR).astype(BF16)
        sums = jnp.dot(turned[...], weights[i % 2][...], preferred_element_type=F32)[0:136]
        if has_state:
            sums = sums + state_ref[at, 0:136, cols] * jnp.exp2((before - top) * FACTOR)
        if last:
            pack_state(out_ref, (s,), cols, sums[0:128], sums[128:129], top)
        else:
            out_ref[s, 0:136, cols] = sums
            out_ref[s, 136:144, cols] = jnp.broadcast_to(top, (8, TILE))


def pack_state(out_ref, lead, cols, weighted, total, top):
    out_ref[(*lead, slice(0, 128), cols)] = weighted.astype(BF16)
    width = top.shape[1]
    line = lax.broadcasted_iota(jnp.int32, (16, width), 0)
    stats = jnp.zeros((16, width), F32)
    for base, value in ((0, top), (3, total)):
        for k in range(3):
            part = value.astype(BF16).astype(F32)
            value = value - part
            stats = jnp.where(line == base + k, jnp.broadcast_to(part, stats.shape), stats)
    out_ref[(*lead, slice(128, 144), cols)] = stats.astype(BF16)


def open_state(ref, lead, cols):
    stats = ref[(*lead, slice(128, 144), cols)].astype(F32)
    top = stats[0:1] + stats[1:2] + stats[2:3]
    total = stats[3:4] + stats[4:5] + stats[5:6]
    return ref[(*lead, slice(0, 128), cols)].astype(F32), total, top


def merge(mine, other):
    top = jnp.maximum(mine[2], other[2])
    a = jnp.exp2((mine[2] - top) * FACTOR)
    b = jnp.exp2((other[2] - top) * FACTOR)
    return mine[0] * a + other[0] * b, mine[1] * a + other[1] * b, top


def join_kernel(state_ref, come_ref, own_ref, out_ref):
    half = COLS // 2
    for e in range(2):
        for side in range(2):
            cols = slice(side * half, (side + 1) * half)
            mine = (state_ref[e, 0:128, cols], state_ref[e, 128:129, cols], state_ref[e, 136:137, cols])
            weighted, total, top = merge(mine, open_state(come_ref, (e,), cols))
            if side == 0:
                own_ref[e, 0:128, :] = weighted
                own_ref[e, 128:136, :] = jnp.broadcast_to(total, (8, half))
                own_ref[e, 136:144, :] = jnp.broadcast_to(top, (8, half))
            else:
                pack_state(out_ref, (e,), slice(0, half), weighted, total, top)


def finish_kernel(own_ref, come_ref, out_ref):
    half = COLS // 2
    everything = slice(0, half)
    for e in range(2):
        mine = (own_ref[e, 0:128, :], own_ref[e, 128:129, :], own_ref[e, 136:137, :])
        weighted, total, _ = merge(mine, open_state(come_ref, (e,), everything))
        mixed = (weighted / total).T.astype(BF16)
        for h in range(HEADS):
            out_ref[e * SPAN : (e + 1) * SPAN, h * HEAD_DIM : (h + 1) * HEAD_DIM] = mixed[
                h * SPAN : (h + 1) * SPAN
            ]


def attend(stacks, sets, blocks, state, last):
    count = len(blocks)
    steps = 2 * len(sets)
    keys = KEYS * count
    kernel = functools.partial(attend_kernel, count, sets, state is not None, last)
    args = [stacks[s] for s in sets] + list(blocks)
    if state is not None:
        args.append(state)
    macs = steps * COLS * keys * (256 + STATE)
    return pl.pallas_call(
        kernel,
        out_shape=jax.ShapeDtypeStruct((steps, STATE, COLS), BF16 if last else F32),
        scratch_shapes=[
            pltpu.VMEM((STATE, keys), BF16),
            pltpu.VMEM((steps, keys, HEAD_DIM), BF16),
            pltpu.VMEM((COLS, HEAD_DIM), BF16),
            pltpu.VMEM((keys, TILE), F32),
            pltpu.VMEM((keys, TILE), F32),
            pltpu.VMEM((keys, TILE), BF16),
            pltpu.VMEM((keys, TILE), BF16),
        ],
        compiler_params=pltpu.CompilerParams(vmem_limit_bytes=32 * 1024 * 1024),
        cost_estimate=pl.CostEstimate(
            flops=4 * macs, bytes_accessed=2**20, transcendentals=steps * COLS * keys
        ),
        name=f"attend_{len(sets)}_{sets[0]}_{count}",
    )(*args)


def call(kernel, out_shape, *args):
    return pl.pallas_call(
        kernel,
        out_shape=out_shape,
        compiler_params=pltpu.CompilerParams(vmem_limit_bytes=16 * 1024 * 1024),
        cost_estimate=pl.CostEstimate(flops=2**21, bytes_accessed=2**20, transcendentals=0),
    )(*args)


def shifted(value, axis, step):
    size = lax.axis_size(axis)
    return lax.ppermute(value, axis, [(i, (i + step) % size) for i in range(size)])


def ids_to_keys(ids):
    size = {a: lax.axis_size(a) for a in AXES}

    def flat(g, z, x, core):
        return ((g * size["z"] + z) * size["x"] + x) * size["core"] + core

    perm = []
    for g in range(8):
        for z in range(8):
            for core in range(2):
                perm.append((flat(g ^ core, g, z // 2, z % 2), flat(g, z, z // 2, core)))
    return lax.ppermute(ids, AXES, perm)


def body(query_rows, key_rows, value_rows, span_ids):
    ids = jnp.broadcast_to(span_ids.astype(F32)[:, None], (2, HEAD_DIM))
    packed = call(
        pack_kernel,
        jax.ShapeDtypeStruct((4, 4, 56, HEAD_DIM), BF16),
        key_rows,
        value_rows,
        ids_to_keys(ids),
    )
    routed = lax.all_to_all(
        packed.reshape(16, 56, HEAD_DIM), ("kv", "x"), 0, 0, tiled=True
    ).reshape(4, 4, 56, HEAD_DIM)
    near = call(spread_kernel, jax.ShapeDtypeStruct((ROWS, HEAD_DIM), BF16), routed)

    right, left = shifted(near, "z", -1), shifted(near, "z", 1)
    rings = [(right, left)]
    beyond = shifted(query_rows, "pair", 1)
    stack = call(
        stack_kernel,
        jax.ShapeDtypeStruct((2, COLS + 16, HEAD_DIM), BF16),
        query_rows,
        beyond,
        ids,
    )
    stacks = (stack, shifted(stack, "core", 1))
    for _ in range(2):
        right, left = shifted(right, "z", -1), shifted(left, "z", 1)
        rings.append((right, left))
    far = shifted(right, "z", -1)

    state = attend(stacks, (0, 1), [near], None, False)
    for pair in rings:
        state = attend(stacks, (0, 1), pair, state, False)
    leaving = attend(stacks, (1,), [far], state, True)
    coming = shifted(leaving, "core", 1)
    mine = attend(stacks, (0,), [far], state, False)
    own, leaving = call(
        join_kernel,
        (
            jax.ShapeDtypeStruct((2, STATE, COLS // 2), F32),
            jax.ShapeDtypeStruct((2, STATE, COLS // 2), BF16),
        ),
        mine,
        coming,
    )
    coming = shifted(leaving, "pair", 1)
    return call(
        finish_kernel, jax.ShapeDtypeStruct((2 * SPAN, HEADS * HEAD_DIM), BF16), own, coming
    )


def solution(mesh):
    split = Mesh(mesh.devices.reshape(4, 2, 8, 4, 2), AXES)
    groups = ("kv", "pair")
    return jax.shard_map(
        body,
        mesh=split,
        in_specs=(P(BLK, groups), P(groups + BLK, None), P(groups + BLK, None), P(BLK)),
        out_specs=P(BLK, groups),
        check_vma=False,
    )
```

```python
import functools
import math

import jax
import jax.numpy as jnp
from jax import lax
from jax.experimental import pallas as pl
from jax.experimental.pallas import tpu as pltpu
from jax.sharding import Mesh
from jax.sharding import PartitionSpec as P


HEAD_DIM = 128
SPAN = 96
PIECE = 24
ROWS = 784
KEYS = 384
HEADS = 4
COLS = 2 * HEADS * SPAN
STATE = 144
TILE = 256
GROUP = 4
MASKED = -1e30
FACTOR = HEAD_DIM**-0.5 * math.log2(math.e)
AXES = ("kv", "pair", "z", "x", "core")
BLK = ("z", "x", "core")
F32 = jnp.float32
BF16 = jnp.bfloat16


def pack_kernel(key_ref, value_ref, out_ref):
    for head in range(4):
        lanes = slice(head * HEAD_DIM, (head + 1) * HEAD_DIM)
        for x in range(4):
            out_ref[head, x, 0:24, :] = key_ref[:, lanes]
            out_ref[head, x, 24:48, :] = value_ref[:, lanes]


def label_kernel(packed_ref, ids_ref, out_ref):
    own = jnp.concatenate([ids_ref[...]] * 4, axis=0).astype(BF16)
    out_ref[:, :, 0:48, :] = packed_ref[...]
    out_ref[:, :, 48:56, :] = jnp.broadcast_to(own[None, None], (4, 4, 8, HEAD_DIM))


def spread_kernel(routed_ref, out_ref):
    for k in range(4):
        for x in range(4):
            at = (k * 4 + x) * PIECE
            out_ref[0, at : at + PIECE, :] = routed_ref[k, x, 0:24, :]
            out_ref[0, KEYS + at : KEYS + at + PIECE, :] = routed_ref[k, x, 24:48, :]
    rows = []
    for k in range(4):
        ids = sum(routed_ref[k, x, 48:56, :].astype(F32) for x in range(4))
        rows += [ids[0:1], ids[0:1], ids[1:2], ids[1:2]]
    out_ref[0, 2 * KEYS : ROWS, :] = jnp.concatenate(rows, axis=0).astype(BF16)


def stack_kernel(own_ref, beyond_ref, ids_ref, out_ref):
    ids = jnp.concatenate([ids_ref[...]] * 8, axis=0).astype(BF16)
    for e in range(2):
        for k in range(2 * HEADS):
            h = k % HEADS
            source = own_ref if k < HEADS else beyond_ref
            out_ref[e, k * SPAN : (k + 1) * SPAN, :] = source[
                e * SPAN : (e + 1) * SPAN, h * HEAD_DIM : (h + 1) * HEAD_DIM
            ]
        out_ref[e, COLS : COLS + 16, :] = ids


def attend_kernel(halves, sets, has_state, last, *refs):
    refs = list(refs)
    q_refs = [refs.pop(0) for _ in sets]
    count = sum(halves)
    given = [refs.pop(0) for _ in halves]
    block = [(g, h, n == 1) for g, n in zip(given, halves) for h in range(n)]
    state_ref = refs.pop(0) if has_state else None
    out_ref, turned, masks, one_hot, *held = refs
    weights, held = held[2:], held[:2]
    keys = KEYS * count

    turned[128:144, :] = jnp.ones((16, keys), BF16)
    for b in range(count):
        turned[0:128, b * KEYS : (b + 1) * KEYS] = block[b][0][block[b][1], KEYS : 2 * KEYS, :].T
    spot = lax.broadcasted_iota(jnp.int32, (SPAN, HEAD_DIM), 0)
    mark = lax.broadcasted_iota(jnp.int32, (SPAN, HEAD_DIM), 1)
    spike = jnp.where(spot == mark, 1.0, 0.0).astype(BF16)
    for k in range(2 * HEADS):
        one_hot[k * SPAN : (k + 1) * SPAN, :] = spike

    lane = lax.broadcasted_iota(jnp.int32, (PIECE, HEAD_DIM), 1)
    row = lax.broadcasted_iota(jnp.int32, (PIECE, HEAD_DIM), 0)
    ahead = (row - lane).astype(F32)
    here = ahead + (lax.axis_index("core") * PIECE).astype(F32)

    def mask(s):
        query_row = q_refs[s // 2][s % 2, COLS : COLS + 16, :].astype(F32)[s % 2 : s % 2 + 1]
        for b in range(count):
            ref, h, own = block[b]
            begin = here if own else ahead + float(h * PIECE)
            places = ref[h, 2 * KEYS : ROWS, :].astype(F32)
            limits = (query_row - places) * float(SPAN)
            for i in range(0, 16, 2):
                pieces = [
                    jnp.where(
                        begin + float(j % 2 * 2 * PIECE)
                        > jnp.broadcast_to(limits[j : j + 1], ahead.shape),
                        MASKED,
                        0.0,
                    )
                    for j in (i, i + 1)
                ]
                at = b * KEYS + i * PIECE
                masks[s, at : at + 2 * PIECE, :] = jnp.concatenate(pieces, axis=0).astype(BF16)

    flip = (((1,), (1,)), ((), ()))
    tiles = [(s, t) for s in range(2 * len(sets)) for t in range(COLS // TILE)]

    def score(i):
        s, t = tiles[i]
        if t == 0:
            mask(s)
        cols = slice(t * TILE, (t + 1) * TILE)
        right = jnp.concatenate([q_refs[s // 2][s % 2, cols, :], one_hot[cols, :]], axis=1)
        best = None
        for b in range(count):
            rows = slice(b * KEYS, (b + 1) * KEYS)
            left = jnp.concatenate([block[b][0][block[b][1], 0:KEYS, :], masks[s, rows, :]], axis=1)
            part = lax.dot_general(left, right, flip, preferred_element_type=F32)
            held[i % 2][rows, :] = part
            peak = jnp.max(part.reshape(KEYS // (8 * GROUP), 8 * GROUP, TILE), axis=0)
            best = peak if best is None else jnp.maximum(best, peak)
            yield best

    for best in score(0):
        pass
    for i, (s, t) in enumerate(tiles):
        cols = slice(t * TILE, (t + 1) * TILE)
        top = jnp.max(best, axis=0, keepdims=True)
        if has_state:
            at = 2 * sets[0] + s
            before = state_ref[at, 136:137, cols]
            top = jnp.maximum(before, top)
        ahead_scores = score(i + 1) if i + 1 < len(tiles) else iter([None] * count)
        for b in range(count):
            rows = slice(b * KEYS, (b + 1) * KEYS)
            weights[i % 2][rows, :] = jnp.exp2((held[i % 2][rows, :] - top) * FACTOR).astype(BF16)
            best = next(ahead_scores)
        sums = jnp.dot(turned[...], weights[i % 2][...], preferred_element_type=F32)[0:136]
        if has_state:
            sums = sums + state_ref[at, 0:136, cols] * jnp.exp2((before - top) * FACTOR)
        if last:
            pack_state(out_ref, (s,), cols, sums[0:128], sums[128:129], top)
        else:
            out_ref[s, 0:136, cols] = sums
            out_ref[s, 136:144, cols] = jnp.broadcast_to(top, (8, TILE))


def pack_state(out_ref, lead, cols, weighted, total, top):
    out_ref[(*lead, slice(0, 128), cols)] = weighted.astype(BF16)
    width = top.shape[1]
    line = lax.broadcasted_iota(jnp.int32, (16, width), 0)
    stats = jnp.zeros((16, width), F32)
    for base, value in ((0, top), (3, total)):
        for k in range(3):
            part = value.astype(BF16).astype(F32)
            value = value - part
            stats = jnp.where(line == base + k, jnp.broadcast_to(part, stats.shape), stats)
    out_ref[(*lead, slice(128, 144), cols)] = stats.astype(BF16)


def open_state(ref, lead, cols):
    stats = ref[(*lead, slice(128, 144), cols)].astype(F32)
    top = stats[0:1] + stats[1:2] + stats[2:3]
    total = stats[3:4] + stats[4:5] + stats[5:6]
    return ref[(*lead, slice(0, 128), cols)].astype(F32), total, top


def merge(mine, other):
    top = jnp.maximum(mine[2], other[2])
    a = jnp.exp2((mine[2] - top) * FACTOR)
    b = jnp.exp2((other[2] - top) * FACTOR)
    return mine[0] * a + other[0] * b, mine[1] * a + other[1] * b, top


def join_kernel(state_ref, come_ref, own_ref, out_ref):
    half = COLS // 2
    for e in range(2):
        for side in range(2):
            cols = slice(side * half, (side + 1) * half)
            mine = (state_ref[e, 0:128, cols], state_ref[e, 128:129, cols], state_ref[e, 136:137, cols])
            weighted, total, top = merge(mine, open_state(come_ref, (e,), cols))
            if side == 0:
                own_ref[e, 0:128, :] = weighted
                own_ref[e, 128:136, :] = jnp.broadcast_to(total, (8, half))
                own_ref[e, 136:144, :] = jnp.broadcast_to(top, (8, half))
            else:
                pack_state(out_ref, (e,), slice(0, half), weighted, total, top)


def finish_kernel(own_ref, come_ref, out_ref):
    half = COLS // 2
    everything = slice(0, half)
    for e in range(2):
        mine = (own_ref[e, 0:128, :], own_ref[e, 128:129, :], own_ref[e, 136:137, :])
        weighted, total, _ = merge(mine, open_state(come_ref, (e,), everything))
        mixed = (weighted / total).T.astype(BF16)
        for h in range(HEADS):
            out_ref[e * SPAN : (e + 1) * SPAN, h * HEAD_DIM : (h + 1) * HEAD_DIM] = mixed[
                h * SPAN : (h + 1) * SPAN
            ]


def attend(stacks, sets, blocks, state, last):
    halves = [block.shape[0] for block in blocks]
    count = sum(halves)
    steps = 2 * len(sets)
    keys = KEYS * count
    kernel = functools.partial(attend_kernel, halves, sets, state is not None, last)
    args = [stacks[s] for s in sets] + list(blocks)
    if state is not None:
        args.append(state)
    macs = steps * COLS * keys * (256 + STATE)
    return pl.pallas_call(
        kernel,
        out_shape=jax.ShapeDtypeStruct((steps, STATE, COLS), BF16 if last else F32),
        scratch_shapes=[
            pltpu.VMEM((STATE, keys), BF16),
            pltpu.VMEM((steps, keys, HEAD_DIM), BF16),
            pltpu.VMEM((COLS, HEAD_DIM), BF16),
            pltpu.VMEM((keys, TILE), F32),
            pltpu.VMEM((keys, TILE), F32),
            pltpu.VMEM((keys, TILE), BF16),
            pltpu.VMEM((keys, TILE), BF16),
        ],
        compiler_params=pltpu.CompilerParams(vmem_limit_bytes=14 * 1024 * 1024),
        cost_estimate=pl.CostEstimate(
            flops=4 * macs, bytes_accessed=2**20, transcendentals=steps * COLS * keys
        ),
    )(*args)


def call(kernel, out_shape, *args):
    return pl.pallas_call(
        kernel,
        out_shape=out_shape,
        compiler_params=pltpu.CompilerParams(vmem_limit_bytes=8 * 1024 * 1024),
        cost_estimate=pl.CostEstimate(flops=2**21, bytes_accessed=2**20, transcendentals=0),
    )(*args)


def around(value):
    zs = lax.axis_size("z")
    perm = []
    for z in range(zs):
        perm.append((2 * z, 2 * ((z - 1) % zs)))
        perm.append((2 * z + 1, 2 * ((z + 1) % zs) + 1))
    return lax.ppermute(value, ("z", "core"), perm)


def shifted(value, axis, step):
    size = lax.axis_size(axis)
    return lax.ppermute(value, axis, [(i, (i + step) % size) for i in range(size)])


def ids_to_keys(ids):
    size = {a: lax.axis_size(a) for a in AXES}

    def flat(g, z, x, core):
        return ((g * size["z"] + z) * size["x"] + x) * size["core"] + core

    perm = []
    for g in range(8):
        for z in range(8):
            for core in range(2):
                perm.append((flat(g ^ core, g, z // 2, z % 2), flat(g, z, z // 2, core)))
    return lax.ppermute(ids, AXES, perm)


def body(query_rows, key_rows, value_rows, span_ids):
    ids = jnp.broadcast_to(span_ids.astype(F32)[:, None], (2, HEAD_DIM))
    packed = call(
        pack_kernel, jax.ShapeDtypeStruct((4, 4, 48, HEAD_DIM), BF16), key_rows, value_rows
    )
    packed = call(
        label_kernel,
        jax.ShapeDtypeStruct((4, 4, 56, HEAD_DIM), BF16),
        packed,
        ids_to_keys(ids),
    ).reshape(16, 56, HEAD_DIM)
    routed = lax.all_to_all(packed, ("kv", "x"), 0, 0, tiled=True)
    routed = routed.reshape(4, 4, 56, HEAD_DIM)
    near = call(spread_kernel, jax.ShapeDtypeStruct((1, ROWS, HEAD_DIM), BF16), routed)
    chip = lax.all_gather(near, "core", axis=0, tiled=True)

    rings = [around(chip)]
    beyond = shifted(query_rows, "pair", 1)
    stack = call(
        stack_kernel,
        jax.ShapeDtypeStruct((2, COLS + 16, HEAD_DIM), BF16),
        query_rows,
        beyond,
        ids,
    )
    stacks = (stack, shifted(stack, "core", 1))
    for _ in range(2):
        rings.append(around(rings[-1]))
    far = around(lax.dynamic_slice_in_dim(rings[-1], lax.axis_index("core"), 1, 0))
    state = None
    for blocks in ([near, rings[0]], [rings[1]], [rings[2]]):
        state = attend(stacks, (0, 1), blocks, state, False)
    leaving = attend(stacks, (1,), [far], state, True)
    coming = shifted(leaving, "core", 1)
    mine = attend(stacks, (0,), [far], state, False)
    own, leaving = call(
        join_kernel,
        (
            jax.ShapeDtypeStruct((2, STATE, COLS // 2), F32),
            jax.ShapeDtypeStruct((2, STATE, COLS // 2), BF16),
        ),
        mine,
        coming,
    )
    coming = shifted(leaving, "pair", 1)
    return call(
        finish_kernel, jax.ShapeDtypeStruct((2 * SPAN, HEADS * HEAD_DIM), BF16), own, coming
    )


def solution(mesh):
    split = Mesh(mesh.devices.reshape(4, 2, 8, 4, 2), AXES)
    groups = ("kv", "pair")
    return jax.shard_map(
        body,
        mesh=split,
        in_specs=(P(BLK, groups), P(groups + BLK, None), P(groups + BLK, None), P(BLK)),
        out_specs=P(BLK, groups),
        check_vma=False,
    )
```

```python
import functools
import math

import jax
import jax.numpy as jnp
from jax import lax
from jax.experimental import pallas as pl
from jax.experimental.pallas import tpu as pltpu
from jax.sharding import Mesh
from jax.sharding import PartitionSpec as P


HEAD_DIM = 128
SPAN = 96
PIECE = 24
ROWS = 784
KEYS = 384
HEADS = 4
COLS = 2 * HEADS * SPAN
STATE = 144
TILE = 256
GROUP = 4
MASKED = -1e30
FACTOR = HEAD_DIM**-0.5 * math.log2(math.e)
AXES = ("kv", "pair", "z", "x", "core")
BLK = ("z", "x", "core")
F32 = jnp.float32
BF16 = jnp.bfloat16


def pack_kernel(key_ref, value_ref, ids_ref, out_ref):
    own = jnp.concatenate([ids_ref[...]] * 4, axis=0).astype(BF16)
    for head in range(4):
        lanes = slice(head * HEAD_DIM, (head + 1) * HEAD_DIM)
        for x in range(4):
            out_ref[head, x, 0:24, :] = key_ref[:, lanes]
            out_ref[head, x, 24:48, :] = value_ref[:, lanes]
            out_ref[head, x, 48:56, :] = own


def spread_kernel(routed_ref, out_ref):
    for k in range(4):
        for x in range(4):
            at = (k * 4 + x) * PIECE
            out_ref[0, at : at + PIECE, :] = routed_ref[k, x, 0:24, :]
            out_ref[0, KEYS + at : KEYS + at + PIECE, :] = routed_ref[k, x, 24:48, :]
    rows = []
    for k in range(4):
        ids = sum(routed_ref[k, x, 48:56, :].astype(F32) for x in range(4))
        rows += [ids[0:1], ids[0:1], ids[1:2], ids[1:2]]
    out_ref[0, 2 * KEYS : ROWS, :] = jnp.concatenate(rows, axis=0).astype(BF16)


def reorder(source, out_ref, first):
    for e in range(2):
        for h in range(HEADS):
            at = first + h * SPAN
            out_ref[e, at : at + SPAN, :] = source[
                e * SPAN : (e + 1) * SPAN, h * HEAD_DIM : (h + 1) * HEAD_DIM
            ]


def reorder_kernel(source_ref, out_ref):
    reorder(source_ref, out_ref, 0)


def stack_kernel(own_ref, beyond_ref, ids_ref, out_ref):
    ids = jnp.concatenate([ids_ref[...]] * 8, axis=0).astype(BF16)
    reorder(beyond_ref, out_ref, COLS // 2)
    for e in range(2):
        out_ref[e, 0 : COLS // 2, :] = own_ref[e]
        out_ref[e, COLS : COLS + 16, :] = ids


def take_kernel(pair_ref, out_ref):
    first = lax.axis_index("core") == 0
    out_ref[0] = jnp.where(first, pair_ref[0], pair_ref[1])


def attend_kernel(halves, sets, has_state, last, *refs):
    refs = list(refs)
    q_refs = [refs.pop(0) for _ in sets]
    count = sum(halves)
    given = [refs.pop(0) for _ in halves]
    block = [(g, h, n == 1) for g, n in zip(given, halves) for h in range(n)]
    state_ref = refs.pop(0) if has_state else None
    out_ref, turned, masks, one_hot, *held = refs
    weights, held = held[2:], held[:2]
    keys = KEYS * count

    turned[128:144, :] = jnp.ones((16, keys), BF16)
    for b in range(count):
        turned[0:128, b * KEYS : (b + 1) * KEYS] = block[b][0][block[b][1], KEYS : 2 * KEYS, :].T
    spot = lax.broadcasted_iota(jnp.int32, (SPAN, HEAD_DIM), 0)
    mark = lax.broadcasted_iota(jnp.int32, (SPAN, HEAD_DIM), 1)
    spike = jnp.where(spot == mark, 1.0, 0.0).astype(BF16)
    for k in range(2 * HEADS):
        one_hot[k * SPAN : (k + 1) * SPAN, :] = spike

    lane = lax.broadcasted_iota(jnp.int32, (PIECE, HEAD_DIM), 1)
    row = lax.broadcasted_iota(jnp.int32, (PIECE, HEAD_DIM), 0)
    ahead = (row - lane).astype(F32)
    here = ahead + (lax.axis_index("core") * PIECE).astype(F32)

    def mask(s):
        query_row = q_refs[s // 2][s % 2, COLS : COLS + 16, :].astype(F32)[s % 2 : s % 2 + 1]
        for b in range(count):
            ref, h, own = block[b]
            begin = here if own else ahead + float(h * PIECE)
            places = ref[h, 2 * KEYS : ROWS, :].astype(F32)
            limits = (query_row - places) * float(SPAN)
            for i in range(0, 16, 2):
                pieces = [
                    jnp.where(
                        begin + float(j % 2 * 2 * PIECE)
                        > jnp.broadcast_to(limits[j : j + 1], ahead.shape),
                        MASKED,
                        0.0,
                    )
                    for j in (i, i + 1)
                ]
                at = b * KEYS + i * PIECE
                masks[s, at : at + 2 * PIECE, :] = jnp.concatenate(pieces, axis=0).astype(BF16)

    flip = (((1,), (1,)), ((), ()))
    tiles = [(s, t) for s in range(2 * len(sets)) for t in range(COLS // TILE)]

    def score(i):
        s, t = tiles[i]
        if t == 0:
            mask(s)
        cols = slice(t * TILE, (t + 1) * TILE)
        right = jnp.concatenate([q_refs[s // 2][s % 2, cols, :], one_hot[cols, :]], axis=1)
        best = None
        for b in range(count):
            rows = slice(b * KEYS, (b + 1) * KEYS)
            left = jnp.concatenate([block[b][0][block[b][1], 0:KEYS, :], masks[s, rows, :]], axis=1)
            part = lax.dot_general(left, right, flip, preferred_element_type=F32)
            held[i % 2][rows, :] = part
            peak = jnp.max(part.reshape(KEYS // (8 * GROUP), 8 * GROUP, TILE), axis=0)
            best = peak if best is None else jnp.maximum(best, peak)
            yield best

    for best in score(0):
        pass
    for i, (s, t) in enumerate(tiles):
        cols = slice(t * TILE, (t + 1) * TILE)
        top = jnp.max(best, axis=0, keepdims=True)
        if has_state:
            at = 2 * sets[0] + s
            before = state_ref[at, 136:137, cols]
            top = jnp.maximum(before, top)
        ahead_scores = score(i + 1) if i + 1 < len(tiles) else iter([None] * count)
        for b in range(count):
            rows = slice(b * KEYS, (b + 1) * KEYS)
            weights[i % 2][rows, :] = jnp.exp2((held[i % 2][rows, :] - top) * FACTOR).astype(BF16)
            best = next(ahead_scores)
        sums = jnp.dot(turned[...], weights[i % 2][...], preferred_element_type=F32)[0:136]
        if has_state:
            sums = sums + state_ref[at, 0:136, cols] * jnp.exp2((before - top) * FACTOR)
        if last:
            pack_state(out_ref, (s,), cols, sums[0:128], sums[128:129], top)
        else:
            out_ref[s, 0:136, cols] = sums
            out_ref[s, 136:144, cols] = jnp.broadcast_to(top, (8, TILE))


def pack_state(out_ref, lead, cols, weighted, total, top):
    out_ref[(*lead, slice(0, 128), cols)] = weighted.astype(BF16)
    width = top.shape[1]
    line = lax.broadcasted_iota(jnp.int32, (16, width), 0)
    stats = jnp.zeros((16, width), F32)
    for base, value in ((0, top), (3, total)):
        for k in range(3):
            part = value.astype(BF16).astype(F32)
            value = value - part
            stats = jnp.where(line == base + k, jnp.broadcast_to(part, stats.shape), stats)
    out_ref[(*lead, slice(128, 144), cols)] = stats.astype(BF16)


def open_state(ref, lead, cols):
    stats = ref[(*lead, slice(128, 144), cols)].astype(F32)
    top = stats[0:1] + stats[1:2] + stats[2:3]
    total = stats[3:4] + stats[4:5] + stats[5:6]
    return ref[(*lead, slice(0, 128), cols)].astype(F32), total, top


def merge(mine, other):
    top = jnp.maximum(mine[2], other[2])
    a = jnp.exp2((mine[2] - top) * FACTOR)
    b = jnp.exp2((other[2] - top) * FACTOR)
    return mine[0] * a + other[0] * b, mine[1] * a + other[1] * b, top


def join_kernel(state_ref, come_ref, own_ref, out_ref):
    half = COLS // 2
    for e in range(2):
        for side in range(2):
            cols = slice(side * half, (side + 1) * half)
            mine = (state_ref[e, 0:128, cols], state_ref[e, 128:129, cols], state_ref[e, 136:137, cols])
            weighted, total, top = merge(mine, open_state(come_ref, (e,), cols))
            if side == 0:
                own_ref[e, 0:128, :] = weighted
                own_ref[e, 128:136, :] = jnp.broadcast_to(total, (8, half))
                own_ref[e, 136:144, :] = jnp.broadcast_to(top, (8, half))
            else:
                pack_state(out_ref, (e,), slice(0, half), weighted, total, top)


def finish_kernel(own_ref, come_ref, out_ref):
    half = COLS // 2
    everything = slice(0, half)
    for e in range(2):
        mine = (own_ref[e, 0:128, :], own_ref[e, 128:129, :], own_ref[e, 136:137, :])
        weighted, total, _ = merge(mine, open_state(come_ref, (e,), everything))
        mixed = (weighted / total).T.astype(BF16)
        for h in range(HEADS):
            out_ref[e * SPAN : (e + 1) * SPAN, h * HEAD_DIM : (h + 1) * HEAD_DIM] = mixed[
                h * SPAN : (h + 1) * SPAN
            ]


def attend(stacks, sets, blocks, state, last):
    halves = [block.shape[0] for block in blocks]
    count = sum(halves)
    steps = 2 * len(sets)
    keys = KEYS * count
    kernel = functools.partial(attend_kernel, halves, sets, state is not None, last)
    args = [stacks[s] for s in sets] + list(blocks)
    if state is not None:
        args.append(state)
    macs = steps * COLS * keys * (256 + STATE)
    return pl.pallas_call(
        kernel,
        out_shape=jax.ShapeDtypeStruct((steps, STATE, COLS), BF16 if last else F32),
        scratch_shapes=[
            pltpu.VMEM((STATE, keys), BF16),
            pltpu.VMEM((steps, keys, HEAD_DIM), BF16),
            pltpu.VMEM((COLS, HEAD_DIM), BF16),
            pltpu.VMEM((keys, TILE), F32),
            pltpu.VMEM((keys, TILE), F32),
            pltpu.VMEM((keys, TILE), BF16),
            pltpu.VMEM((keys, TILE), BF16),
        ],
        compiler_params=pltpu.CompilerParams(vmem_limit_bytes=14 * 1024 * 1024),
        cost_estimate=pl.CostEstimate(
            flops=4 * macs, bytes_accessed=2**20, transcendentals=steps * COLS * keys
        ),
    )(*args)


def call(kernel, out_shape, *args):
    return pl.pallas_call(
        kernel,
        out_shape=out_shape,
        compiler_params=pltpu.CompilerParams(vmem_limit_bytes=8 * 1024 * 1024),
        cost_estimate=pl.CostEstimate(flops=2**21, bytes_accessed=2**20, transcendentals=0),
    )(*args)


def around(value):
    zs = lax.axis_size("z")
    perm = []
    for z in range(zs):
        perm.append((2 * z, 2 * ((z - 1) % zs)))
        perm.append((2 * z + 1, 2 * ((z + 1) % zs) + 1))
    return lax.ppermute(value, ("z", "core"), perm)


def shifted(value, axis, step):
    size = lax.axis_size(axis)
    return lax.ppermute(value, axis, [(i, (i + step) % size) for i in range(size)])


def ids_to_keys(ids):
    size = {a: lax.axis_size(a) for a in AXES}

    def flat(g, z, x, core):
        return ((g * size["z"] + z) * size["x"] + x) * size["core"] + core

    perm = []
    for g in range(8):
        for z in range(8):
            for core in range(2):
                perm.append((flat(g ^ core, g, z // 2, z % 2), flat(g, z, z // 2, core)))
    return lax.ppermute(ids, AXES, perm)


def body(query_rows, key_rows, value_rows, span_ids):
    ids = jnp.broadcast_to(span_ids.astype(F32)[:, None], (2, HEAD_DIM))
    places = ids_to_keys(ids)
    packed = call(
        pack_kernel,
        jax.ShapeDtypeStruct((4, 4, 56, HEAD_DIM), BF16),
        key_rows,
        value_rows,
        places,
    ).reshape(16, 56, HEAD_DIM)
    routed = lax.all_to_all(packed, ("kv", "x"), 0, 0, tiled=True)
    routed = routed.reshape(4, 4, 56, HEAD_DIM)
    near = call(spread_kernel, jax.ShapeDtypeStruct((1, ROWS, HEAD_DIM), BF16), routed)
    chip = lax.all_gather(near, "core", axis=0, tiled=True)

    rings = [around(chip)]
    beyond = shifted(query_rows, "pair", 1)
    own = call(
        reorder_kernel, jax.ShapeDtypeStruct((2, COLS // 2, HEAD_DIM), BF16), query_rows
    )
    stack = call(
        stack_kernel,
        jax.ShapeDtypeStruct((2, COLS + 16, HEAD_DIM), BF16),
        own,
        beyond,
        ids,
    )
    stacks = (stack, shifted(stack, "core", 1))
    for _ in range(2):
        rings.append(around(rings[-1]))
    far = around(call(take_kernel, jax.ShapeDtypeStruct(near.shape, BF16), rings[2]))
    state = None
    for blocks in ([near, rings[0]], [rings[1]], [rings[2]]):
        state = attend(stacks, (0, 1), blocks, state, False)
    leaving = attend(stacks, (1,), [far], state, True)
    coming = shifted(leaving, "core", 1)
    mine = attend(stacks, (0,), [far], state, False)
    own, leaving = call(
        join_kernel,
        (
            jax.ShapeDtypeStruct((2, STATE, COLS // 2), F32),
            jax.ShapeDtypeStruct((2, STATE, COLS // 2), BF16),
        ),
        mine,
        coming,
    )
    coming = shifted(leaving, "pair", 1)
    return call(
        finish_kernel, jax.ShapeDtypeStruct((2 * SPAN, HEADS * HEAD_DIM), BF16), own, coming
    )


def solution(mesh):
    split = Mesh(mesh.devices.reshape(4, 2, 8, 4, 2), AXES)
    groups = ("kv", "pair")
    return jax.shard_map(
        body,
        mesh=split,
        in_specs=(P(BLK, groups), P(groups + BLK, None), P(groups + BLK, None), P(BLK)),
        out_specs=P(BLK, groups),
        check_vma=False,
    )
```

```python
import functools
import math

import jax
import jax.numpy as jnp
from jax import lax
from jax.experimental import pallas as pl
from jax.experimental.pallas import tpu as pltpu
from jax.sharding import Mesh
from jax.sharding import PartitionSpec as P


HEAD_DIM = 128
SPAN = 96
PIECE = 24
ROWS = 784
KEYS = 384
HEADS = 4
COLS = 2 * HEADS * SPAN
STATE = 144
PART = 256
GROUP = 4
MASKED = -1e30
FACTOR = HEAD_DIM**-0.5 * math.log2(math.e)
AXES = ("kv", "pair", "z", "x", "core")
BLK = ("z", "x", "core")
F32 = jnp.float32
BF16 = jnp.bfloat16


def pack_kernel(key_ref, value_ref, ids_ref, out_ref):
    own = jnp.concatenate([ids_ref[...]] * 4, axis=0).astype(BF16)
    for head in range(4):
        lanes = slice(head * HEAD_DIM, (head + 1) * HEAD_DIM)
        for x in range(4):
            out_ref[head, x, 0:24, :] = key_ref[:, lanes]
            out_ref[head, x, 24:48, :] = value_ref[:, lanes]
            out_ref[head, x, 48:56, :] = own


def spread_kernel(routed_ref, out_ref):
    for k in range(4):
        for x in range(4):
            at = (k * 4 + x) * PIECE
            out_ref[0, at : at + PIECE, :] = routed_ref[k, x, 0:24, :]
            out_ref[0, KEYS + at : KEYS + at + PIECE, :] = routed_ref[k, x, 24:48, :]
    rows = []
    for k in range(4):
        ids = sum(routed_ref[k, x, 48:56, :].astype(F32) for x in range(4))
        rows += [ids[0:1], ids[0:1], ids[1:2], ids[1:2]]
    out_ref[0, 2 * KEYS : ROWS, :] = jnp.concatenate(rows, axis=0).astype(BF16)


def reorder(source, out_ref, first):
    for e in range(2):
        for h in range(HEADS):
            at = first + h * SPAN
            out_ref[e, at : at + SPAN, :] = source[
                e * SPAN : (e + 1) * SPAN, h * HEAD_DIM : (h + 1) * HEAD_DIM
            ]


def reorder_kernel(source_ref, out_ref):
    reorder(source_ref, out_ref, 0)


def stack_kernel(own_ref, beyond_ref, ids_ref, out_ref):
    ids = jnp.concatenate([ids_ref[...]] * 8, axis=0).astype(BF16)
    reorder(beyond_ref, out_ref, COLS // 2)
    for e in range(2):
        out_ref[e, 0 : COLS // 2, :] = own_ref[e]
        out_ref[e, COLS : COLS + 16, :] = ids


def attend_kernel(mine, sets, start, width, has_state, last, *refs):
    refs = list(refs)
    q_refs = [refs.pop(0) for _ in sets]
    count = len(mine)
    block = [refs.pop(0) for _ in mine]
    state_ref = refs.pop(0) if has_state else None
    out_ref, turned, masks, one_hot, *held = refs
    weights, held = held[2:], held[:2]
    keys = KEYS * count

    turned[128:144, :] = jnp.ones((16, keys), BF16)
    for b in range(count):
        turned[0:128, b * KEYS : (b + 1) * KEYS] = block[b][0, KEYS : 2 * KEYS, :].T
    spot = lax.broadcasted_iota(jnp.int32, (SPAN, HEAD_DIM), 0)
    mark = lax.broadcasted_iota(jnp.int32, (SPAN, HEAD_DIM), 1)
    spike = jnp.where(spot == mark, 1.0, 0.0).astype(BF16)
    for k in range(2 * HEADS):
        one_hot[k * SPAN : (k + 1) * SPAN, :] = spike

    lane = lax.broadcasted_iota(jnp.int32, (PIECE, HEAD_DIM), 1)
    row = lax.broadcasted_iota(jnp.int32, (PIECE, HEAD_DIM), 0)
    ahead = (row - lane).astype(F32)
    core = lax.axis_index("core")

    def mask(s):
        query_row = q_refs[s // 2][s % 2, COLS : COLS + 16, :].astype(F32)[s % 2 : s % 2 + 1]
        for b in range(count):
            begin = ahead + ((core if mine[b] else 1 - core) * PIECE).astype(F32)
            places = block[b][0, 2 * KEYS : ROWS, :].astype(F32)
            limits = (query_row - places) * float(SPAN)
            for i in range(0, 16, 2):
                pieces = [
                    jnp.where(
                        begin + float(j % 2 * 2 * PIECE)
                        > jnp.broadcast_to(limits[j : j + 1], ahead.shape),
                        MASKED,
                        0.0,
                    )
                    for j in (i, i + 1)
                ]
                at = b * KEYS + i * PIECE
                masks[s, at : at + 2 * PIECE, :] = jnp.concatenate(pieces, axis=0).astype(BF16)

    flip = (((1,), (1,)), ((), ()))
    spans = 2 * len(sets)
    taken = slice(start, start + width)

    def score(s):
        mask(s)
        right = jnp.concatenate([q_refs[s // 2][s % 2, taken, :], one_hot[taken, :]], axis=1)
        best = None
        for b in range(count):
            rows = slice(b * KEYS, (b + 1) * KEYS)
            left = jnp.concatenate([block[b][0, 0:KEYS, :], masks[s, rows, :]], axis=1)
            part = lax.dot_general(left, right, flip, preferred_element_type=F32)
            held[s % 2][rows, :] = part
            peak = jnp.max(part.reshape(KEYS // (8 * GROUP), 8 * GROUP, width), axis=0)
            best = peak if best is None else jnp.maximum(best, peak)
        return best

    best = score(0)
    for s in range(spans):
        top = jnp.max(best, axis=0, keepdims=True)
        at = 2 * sets[0] + s
        if has_state:
            before = state_ref[at, 136:137, taken]
            top = jnp.maximum(before, top)
        for b in range(count):
            rows = slice(b * KEYS, (b + 1) * KEYS)
            weights[s % 2][rows, :] = jnp.exp2((held[s % 2][rows, :] - top) * FACTOR).astype(BF16)
        if s + 1 < spans:
            best = score(s + 1)
        for first in range(0, width, PART):
            inner = slice(first, min(first + PART, width))
            outer = slice(start + inner.start, start + inner.stop)
            sums = jnp.dot(turned[...], weights[s % 2][:, inner], preferred_element_type=F32)[0:136]
            peak = top[:, inner]
            if has_state:
                shrink = jnp.exp2((before[:, inner] - peak) * FACTOR)
                sums = sums + state_ref[at, 0:136, outer] * shrink
            if last:
                pack_state(out_ref, (s,), inner, sums[0:128], sums[128:129], peak)
            else:
                out_ref[s, 0:136, inner] = sums
                out_ref[s, 136:144, inner] = jnp.broadcast_to(peak, (8, peak.shape[1]))


def pack_state(out_ref, lead, cols, weighted, total, top):
    out_ref[(*lead, slice(0, 128), cols)] = weighted.astype(BF16)
    width = top.shape[1]
    line = lax.broadcasted_iota(jnp.int32, (16, width), 0)
    stats = jnp.zeros((16, width), F32)
    for base, value in ((0, top), (3, total)):
        for k in range(3):
            part = value.astype(BF16).astype(F32)
            value = value - part
            stats = jnp.where(line == base + k, jnp.broadcast_to(part, stats.shape), stats)
    out_ref[(*lead, slice(128, 144), cols)] = stats.astype(BF16)


def open_state(ref, lead, cols):
    stats = ref[(*lead, slice(128, 144), cols)].astype(F32)
    top = stats[0:1] + stats[1:2] + stats[2:3]
    total = stats[3:4] + stats[4:5] + stats[5:6]
    return ref[(*lead, slice(0, 128), cols)].astype(F32), total, top


def merge(mine, other):
    top = jnp.maximum(mine[2], other[2])
    a = jnp.exp2((mine[2] - top) * FACTOR)
    b = jnp.exp2((other[2] - top) * FACTOR)
    return mine[0] * a + other[0] * b, mine[1] * a + other[1] * b, top


def read_state(ref, e):
    return ref[e, 0:128, :], ref[e, 128:129, :], ref[e, 136:137, :]


def join_kernel(mine_ref, come_ref, out_ref):
    every = slice(0, COLS // 2)
    for e in range(2):
        merged = merge(read_state(mine_ref, e), open_state(come_ref, (e,), every))
        pack_state(out_ref, (e,), every, *merged)


def finish_kernel(mine_ref, core_ref, plane_ref, out_ref):
    every = slice(0, COLS // 2)
    for e in range(2):
        merged = merge(read_state(mine_ref, e), open_state(core_ref, (e,), every))
        weighted, total, _ = merge(merged, open_state(plane_ref, (e,), every))
        mixed = (weighted / total).T.astype(BF16)
        for h in range(HEADS):
            out_ref[e * SPAN : (e + 1) * SPAN, h * HEAD_DIM : (h + 1) * HEAD_DIM] = mixed[
                h * SPAN : (h + 1) * SPAN
            ]


def attend(stacks, sets, blocks, mine, state, last, start=0, width=COLS):
    count = len(blocks)
    steps = 2 * len(sets)
    keys = KEYS * count
    kernel = functools.partial(
        attend_kernel, mine, sets, start, width, state is not None, last
    )
    args = [stacks[s] for s in sets] + list(blocks)
    if state is not None:
        args.append(state)
    macs = steps * width * keys * (256 + STATE)
    return pl.pallas_call(
        kernel,
        out_shape=jax.ShapeDtypeStruct((steps, STATE, width), BF16 if last else F32),
        scratch_shapes=[
            pltpu.VMEM((STATE, keys), BF16),
            pltpu.VMEM((steps, keys, HEAD_DIM), BF16),
            pltpu.VMEM((COLS, HEAD_DIM), BF16),
            pltpu.VMEM((keys, width), F32),
            pltpu.VMEM((keys, width), F32),
            pltpu.VMEM((keys, width), BF16),
            pltpu.VMEM((keys, width), BF16),
        ],
        compiler_params=pltpu.CompilerParams(vmem_limit_bytes=14 * 1024 * 1024),
        cost_estimate=pl.CostEstimate(
            flops=4 * macs, bytes_accessed=2**20, transcendentals=steps * width * keys
        ),
    )(*args)


def call(kernel, out_shape, *args):
    return pl.pallas_call(
        kernel,
        out_shape=out_shape,
        compiler_params=pltpu.CompilerParams(vmem_limit_bytes=8 * 1024 * 1024),
        cost_estimate=pl.CostEstimate(flops=2**21, bytes_accessed=2**20, transcendentals=0),
    )(*args)


def around(value):
    zs = lax.axis_size("z")
    perm = []
    for z in range(zs):
        perm.append((2 * z, 2 * ((z - 1) % zs)))
        perm.append((2 * z + 1, 2 * ((z + 1) % zs) + 1))
    return lax.ppermute(value, ("z", "core"), perm)


def shifted(value, axis, step):
    size = lax.axis_size(axis)
    return lax.ppermute(value, axis, [(i, (i + step) % size) for i in range(size)])


def ids_to_keys(ids):
    size = {a: lax.axis_size(a) for a in AXES}

    def flat(g, z, x, core):
        return ((g * size["z"] + z) * size["x"] + x) * size["core"] + core

    perm = []
    for g in range(8):
        for z in range(8):
            for core in range(2):
                perm.append((flat(g ^ core, g, z // 2, z % 2), flat(g, z, z // 2, core)))
    return lax.ppermute(ids, AXES, perm)


def body(query_rows, key_rows, value_rows, span_ids):
    ids = jnp.broadcast_to(span_ids.astype(F32)[:, None], (2, HEAD_DIM))
    places = ids_to_keys(ids)
    packed = call(
        pack_kernel,
        jax.ShapeDtypeStruct((4, 4, 56, HEAD_DIM), BF16),
        key_rows,
        value_rows,
        places,
    ).reshape(16, 56, HEAD_DIM)
    routed = lax.all_to_all(packed, ("kv", "x"), 0, 0, tiled=True)
    routed = routed.reshape(4, 4, 56, HEAD_DIM)
    near = call(spread_kernel, jax.ShapeDtypeStruct((1, ROWS, HEAD_DIM), BF16), routed)
    beyond = shifted(query_rows, "pair", 1)
    own = call(
        reorder_kernel, jax.ShapeDtypeStruct((2, COLS // 2, HEAD_DIM), BF16), query_rows
    )
    stack = call(
        stack_kernel,
        jax.ShapeDtypeStruct((2, COLS + 16, HEAD_DIM), BF16),
        own,
        beyond,
        ids,
    )
    stacks = (stack, shifted(stack, "core", 1))
    own_line, other_line = [], []
    own_line.append(around(near))
    mate = shifted(near, "core", 1)
    other_line.append(around(mate))
    for k in range(1, 4):
        own_line.append(around(own_line[-1]))
        if k < 3:
            other_line.append(around(other_line[-1]))
    state = attend(stacks, (0, 1), [near], [True], None, False)
    for k in range(3):
        both = [own_line[k], other_line[k]]
        state = attend(stacks, (0, 1), both, [True, False], state, False)
    far = own_line[3]
    half = COLS // 2
    packed_half = jax.ShapeDtypeStruct((2, STATE, half), BF16)
    leaving = attend(stacks, (1,), [far], [True], state, True, half, half)
    coming = shifted(leaving, "core", 1)
    mine = attend(stacks, (0,), [far], [True], state, False, half, half)
    joined = call(join_kernel, packed_half, mine, coming)
    plane = shifted(joined, "pair", 1)
    leaving = attend(stacks, (1,), [far], [True], state, True, 0, half)
    coming = shifted(leaving, "core", 1)
    mine = attend(stacks, (0,), [far], [True], state, False, 0, half)
    return call(
        finish_kernel,
        jax.ShapeDtypeStruct((2 * SPAN, HEADS * HEAD_DIM), BF16),
        mine,
        coming,
        plane,
    )


def solution(mesh):
    split = Mesh(mesh.devices.reshape(4, 2, 8, 4, 2), AXES)
    groups = ("kv", "pair")
    return jax.shard_map(
        body,
        mesh=split,
        in_specs=(P(BLK, groups), P(groups + BLK, None), P(groups + BLK, None), P(BLK)),
        out_specs=P(BLK, groups),
        check_vma=False,
    )
```

```python
import functools
import math

import jax
import jax.numpy as jnp
from jax import lax
from jax.experimental import pallas as pl
from jax.experimental.pallas import tpu as pltpu
from jax.sharding import Mesh
from jax.sharding import PartitionSpec as P


HEAD_DIM = 128
SPAN = 96
PIECE = 24
ROWS = 784
KEYS = 384
HEADS = 4
COLS = 2 * HEADS * SPAN
STATE = 144
PART = 256
GROUP = 4
MASKED = -1e30
FACTOR = HEAD_DIM**-0.5 * math.log2(math.e)
AXES = ("kv", "pair", "z", "x", "core")
BLK = ("z", "x", "core")
F32 = jnp.float32
BF16 = jnp.bfloat16


def pack_kernel(key_ref, value_ref, ids_ref, out_ref):
    own = jnp.concatenate([ids_ref[...]] * 4, axis=0).astype(BF16)
    for head in range(4):
        lanes = slice(head * HEAD_DIM, (head + 1) * HEAD_DIM)
        for x in range(4):
            out_ref[head, x, 0:24, :] = key_ref[:, lanes]
            out_ref[head, x, 24:48, :] = value_ref[:, lanes]
            out_ref[head, x, 48:56, :] = own


def spread_kernel(routed_ref, out_ref):
    for k in range(4):
        for x in range(4):
            at = (k * 4 + x) * PIECE
            out_ref[0, at : at + PIECE, :] = routed_ref[k, x, 0:24, :]
            out_ref[0, KEYS + at : KEYS + at + PIECE, :] = routed_ref[k, x, 24:48, :]
    rows = []
    for k in range(4):
        ids = sum(routed_ref[k, x, 48:56, :].astype(F32) for x in range(4))
        rows += [ids[0:1], ids[0:1], ids[1:2], ids[1:2]]
    out_ref[0, 2 * KEYS : ROWS, :] = jnp.concatenate(rows, axis=0).astype(BF16)


def reorder(source, out_ref, first):
    for e in range(2):
        for h in range(HEADS):
            at = first + h * SPAN
            out_ref[e, at : at + SPAN, :] = source[
                e * SPAN : (e + 1) * SPAN, h * HEAD_DIM : (h + 1) * HEAD_DIM
            ]


def reorder_kernel(source_ref, out_ref):
    reorder(source_ref, out_ref, 0)


def stack_kernel(own_ref, beyond_ref, ids_ref, out_ref):
    ids = jnp.concatenate([ids_ref[...]] * 8, axis=0).astype(BF16)
    reorder(beyond_ref, out_ref, COLS // 2)
    for e in range(2):
        out_ref[e, 0 : COLS // 2, :] = own_ref[e]
        out_ref[e, COLS : COLS + 16, :] = ids


def attend_kernel(mine, sets, start, width, has_state, last, *refs):
    refs = list(refs)
    q_refs = [refs.pop(0) for _ in sets]
    count = len(mine)
    block = [refs.pop(0) for _ in mine]
    state_ref = refs.pop(0) if has_state else None
    out_ref, turned, masks, one_hot, *held = refs
    weights, held = held[2:], held[:2]
    keys = KEYS * count

    turned[128:144, :] = jnp.ones((16, keys), BF16)
    for b in range(count):
        turned[0:128, b * KEYS : (b + 1) * KEYS] = block[b][0, KEYS : 2 * KEYS, :].T
    spot = lax.broadcasted_iota(jnp.int32, (SPAN, HEAD_DIM), 0)
    mark = lax.broadcasted_iota(jnp.int32, (SPAN, HEAD_DIM), 1)
    spike = jnp.where(spot == mark, 1.0, 0.0).astype(BF16)
    for k in range(2 * HEADS):
        one_hot[k * SPAN : (k + 1) * SPAN, :] = spike

    lane = lax.broadcasted_iota(jnp.int32, (PIECE, HEAD_DIM), 1)
    row = lax.broadcasted_iota(jnp.int32, (PIECE, HEAD_DIM), 0)
    ahead = (row - lane).astype(F32)
    core = lax.axis_index("core")

    def mask(s):
        query_row = q_refs[s // 2][s % 2, COLS : COLS + 16, :].astype(F32)[s % 2 : s % 2 + 1]
        for b in range(count):
            begin = ahead + ((core if mine[b] else 1 - core) * PIECE).astype(F32)
            places = block[b][0, 2 * KEYS : ROWS, :].astype(F32)
            limits = (query_row - places) * float(SPAN)
            for i in range(0, 16, 2):
                pieces = [
                    jnp.where(
                        begin + float(j % 2 * 2 * PIECE)
                        > jnp.broadcast_to(limits[j : j + 1], ahead.shape),
                        MASKED,
                        0.0,
                    )
                    for j in (i, i + 1)
                ]
                at = b * KEYS + i * PIECE
                masks[s, at : at + 2 * PIECE, :] = jnp.concatenate(pieces, axis=0).astype(BF16)

    flip = (((1,), (1,)), ((), ()))
    spans = 2 * len(sets)
    taken = slice(start, start + width)

    def score(s):
        mask(s)
        right = jnp.concatenate([q_refs[s // 2][s % 2, taken, :], one_hot[taken, :]], axis=1)
        best = None
        for b in range(count):
            rows = slice(b * KEYS, (b + 1) * KEYS)
            left = jnp.concatenate([block[b][0, 0:KEYS, :], masks[s, rows, :]], axis=1)
            part = lax.dot_general(left, right, flip, preferred_element_type=F32)
            held[s % 2][rows, :] = part
            peak = jnp.max(part.reshape(KEYS // (8 * GROUP), 8 * GROUP, width), axis=0)
            best = peak if best is None else jnp.maximum(best, peak)
        return best

    best = score(0)
    for s in range(spans):
        top = jnp.max(best, axis=0, keepdims=True)
        at = 2 * sets[0] + s
        if has_state:
            before = state_ref[at, 136:137, taken]
            top = jnp.maximum(before, top)
        for b in range(count):
            rows = slice(b * KEYS, (b + 1) * KEYS)
            weights[s % 2][rows, :] = jnp.exp2((held[s % 2][rows, :] - top) * FACTOR).astype(BF16)
        if s + 1 < spans:
            best = score(s + 1)
        for first in range(0, width, PART):
            inner = slice(first, min(first + PART, width))
            outer = slice(start + inner.start, start + inner.stop)
            sums = jnp.dot(turned[...], weights[s % 2][:, inner], preferred_element_type=F32)[0:136]
            peak = top[:, inner]
            if has_state:
                shrink = jnp.exp2((before[:, inner] - peak) * FACTOR)
                sums = sums + state_ref[at, 0:136, outer] * shrink
            if last:
                pack_state(out_ref, (s,), inner, sums[0:128], sums[128:129], peak)
            else:
                out_ref[s, 0:136, inner] = sums
                out_ref[s, 136:144, inner] = jnp.broadcast_to(peak, (8, peak.shape[1]))


def pack_state(out_ref, lead, cols, weighted, total, top):
    out_ref[(*lead, slice(0, 128), cols)] = weighted.astype(BF16)
    width = top.shape[1]
    line = lax.broadcasted_iota(jnp.int32, (16, width), 0)
    stats = jnp.zeros((16, width), F32)
    for base, value in ((0, top), (3, total)):
        for k in range(3):
            part = value.astype(BF16).astype(F32)
            value = value - part
            stats = jnp.where(line == base + k, jnp.broadcast_to(part, stats.shape), stats)
    out_ref[(*lead, slice(128, 144), cols)] = stats.astype(BF16)


def open_state(ref, lead, cols):
    stats = ref[(*lead, slice(128, 144), cols)].astype(F32)
    top = stats[0:1] + stats[1:2] + stats[2:3]
    total = stats[3:4] + stats[4:5] + stats[5:6]
    return ref[(*lead, slice(0, 128), cols)].astype(F32), total, top


def merge(mine, other):
    top = jnp.maximum(mine[2], other[2])
    a = jnp.exp2((mine[2] - top) * FACTOR)
    b = jnp.exp2((other[2] - top) * FACTOR)
    return mine[0] * a + other[0] * b, mine[1] * a + other[1] * b, top


def read_state(ref, e):
    return ref[e, 0:128, :], ref[e, 128:129, :], ref[e, 136:137, :]


def join_kernel(mine_ref, come_ref, out_ref):
    every = slice(0, COLS // 2)
    for e in range(2):
        merged = merge(read_state(mine_ref, e), open_state(come_ref, (e,), every))
        pack_state(out_ref, (e,), every, *merged)


def finish_kernel(mine_ref, core_ref, plane_ref, out_ref):
    every = slice(0, COLS // 2)
    for e in range(2):
        merged = merge(read_state(mine_ref, e), open_state(core_ref, (e,), every))
        weighted, total, _ = merge(merged, open_state(plane_ref, (e,), every))
        mixed = (weighted / total).T.astype(BF16)
        for h in range(HEADS):
            out_ref[e * SPAN : (e + 1) * SPAN, h * HEAD_DIM : (h + 1) * HEAD_DIM] = mixed[
                h * SPAN : (h + 1) * SPAN
            ]


def attend(stacks, sets, blocks, mine, state, last, start=0, width=COLS):
    count = len(blocks)
    steps = 2 * len(sets)
    keys = KEYS * count
    kernel = functools.partial(
        attend_kernel, mine, sets, start, width, state is not None, last
    )
    args = [stacks[s] for s in sets] + list(blocks)
    if state is not None:
        args.append(state)
    macs = steps * width * keys * (256 + STATE)
    return pl.pallas_call(
        kernel,
        out_shape=jax.ShapeDtypeStruct((steps, STATE, width), BF16 if last else F32),
        scratch_shapes=[
            pltpu.VMEM((STATE, keys), BF16),
            pltpu.VMEM((steps, keys, HEAD_DIM), BF16),
            pltpu.VMEM((COLS, HEAD_DIM), BF16),
            pltpu.VMEM((keys, width), F32),
            pltpu.VMEM((keys, width), F32),
            pltpu.VMEM((keys, width), BF16),
            pltpu.VMEM((keys, width), BF16),
        ],
        compiler_params=pltpu.CompilerParams(vmem_limit_bytes=14 * 1024 * 1024),
        cost_estimate=pl.CostEstimate(
            flops=4 * macs, bytes_accessed=2**20, transcendentals=steps * width * keys
        ),
    )(*args)


def call(kernel, out_shape, *args):
    return pl.pallas_call(
        kernel,
        out_shape=out_shape,
        compiler_params=pltpu.CompilerParams(vmem_limit_bytes=8 * 1024 * 1024),
        cost_estimate=pl.CostEstimate(flops=2**21, bytes_accessed=2**20, transcendentals=0),
    )(*args)


def around(value):
    zs = lax.axis_size("z")
    perm = []
    for z in range(zs):
        perm.append((2 * z, 2 * ((z - 1) % zs)))
        perm.append((2 * z + 1, 2 * ((z + 1) % zs) + 1))
    return lax.ppermute(value, ("z", "core"), perm)


def shifted(value, axis, step):
    size = lax.axis_size(axis)
    return lax.ppermute(value, axis, [(i, (i + step) % size) for i in range(size)])


def ids_to_keys(ids):
    size = {a: lax.axis_size(a) for a in AXES}

    def flat(g, z, x, core):
        return ((g * size["z"] + z) * size["x"] + x) * size["core"] + core

    perm = []
    for g in range(8):
        for z in range(8):
            for core in range(2):
                perm.append((flat(g ^ core, g, z // 2, z % 2), flat(g, z, z // 2, core)))
    return lax.ppermute(ids, AXES, perm)


def body(query_rows, key_rows, value_rows, span_ids):
    ids = jnp.broadcast_to(span_ids.astype(F32)[:, None], (2, HEAD_DIM))
    places = ids_to_keys(ids)
    packed = call(
        pack_kernel,
        jax.ShapeDtypeStruct((4, 4, 56, HEAD_DIM), BF16),
        key_rows,
        value_rows,
        places,
    ).reshape(16, 56, HEAD_DIM)
    routed = lax.all_to_all(packed, ("kv", "x"), 0, 0, tiled=True)
    routed = routed.reshape(4, 4, 56, HEAD_DIM)
    near = call(spread_kernel, jax.ShapeDtypeStruct((1, ROWS, HEAD_DIM), BF16), routed)
    beyond = shifted(query_rows, "pair", 1)
    own = call(
        reorder_kernel, jax.ShapeDtypeStruct((2, COLS // 2, HEAD_DIM), BF16), query_rows
    )
    stack = call(
        stack_kernel,
        jax.ShapeDtypeStruct((2, COLS + 16, HEAD_DIM), BF16),
        own,
        beyond,
        ids,
    )
    stacks = (stack, shifted(stack, "core", 1))
    own_line, other_line = [], []
    own_line.append(around(near))
    mate = shifted(near, "core", 1)
    other_line.append(around(mate))
    for k in range(1, 4):
        own_line.append(around(own_line[-1]))
        if k < 3:
            other_line.append(around(other_line[-1]))
    state = None
    parts = [
        ([near, own_line[0]], [True, True]),
        ([other_line[0], own_line[1]], [False, True]),
        ([other_line[1], own_line[2]], [False, True]),
        ([other_line[2]], [False]),
    ]
    for blocks, mine in parts:
        state = attend(stacks, (0, 1), blocks, mine, state, False)
    far = own_line[3]
    half = COLS // 2
    packed_half = jax.ShapeDtypeStruct((2, STATE, half), BF16)
    leaving = attend(stacks, (1,), [far], [True], state, True, half, half)
    coming = shifted(leaving, "core", 1)
    mine = attend(stacks, (0,), [far], [True], state, False, half, half)
    joined = call(join_kernel, packed_half, mine, coming)
    plane = shifted(joined, "pair", 1)
    leaving = attend(stacks, (1,), [far], [True], state, True, 0, half)
    coming = shifted(leaving, "core", 1)
    mine = attend(stacks, (0,), [far], [True], state, False, 0, half)
    return call(
        finish_kernel,
        jax.ShapeDtypeStruct((2 * SPAN, HEADS * HEAD_DIM), BF16),
        mine,
        coming,
        plane,
    )


def solution(mesh):
    split = Mesh(mesh.devices.reshape(4, 2, 8, 4, 2), AXES)
    groups = ("kv", "pair")
    return jax.shard_map(
        body,
        mesh=split,
        in_specs=(P(BLK, groups), P(groups + BLK, None), P(groups + BLK, None), P(BLK)),
        out_specs=P(BLK, groups),
        check_vma=False,
    )
```

```python
import functools
import math

import jax
import jax.numpy as jnp
from jax import lax
from jax.experimental import pallas as pl
from jax.experimental.pallas import tpu as pltpu
from jax.sharding import Mesh
from jax.sharding import PartitionSpec as P


HEAD_DIM = 128
SPAN = 96
PIECE = 24
ROWS = 784
KEYS = 384
HEADS = 4
COLS = 2 * HEADS * SPAN
STATE = 144
PART = 256
GROUP = 4
MASKED = -1e30
FACTOR = HEAD_DIM**-0.5 * math.log2(math.e)
AXES = ("kv", "pair", "z", "x", "core")
BLK = ("z", "x", "core")
F32 = jnp.float32
BF16 = jnp.bfloat16


def id_rows(ids_ref, rows):
    line = lax.broadcasted_iota(jnp.int32, (rows, HEAD_DIM), 0)
    return jnp.where(line % 2 == 0, ids_ref[0], ids_ref[1]).astype(F32).astype(BF16)


def pack_kernel(key_ref, value_ref, ids_ref, out_ref):
    own = id_rows(ids_ref, 8)
    for head in range(4):
        lanes = slice(head * HEAD_DIM, (head + 1) * HEAD_DIM)
        for x in range(4):
            out_ref[head, x, 0:24, :] = key_ref[:, lanes]
            out_ref[head, x, 24:48, :] = value_ref[:, lanes]
            out_ref[head, x, 48:56, :] = own


def spread_kernel(routed_ref, out_ref):
    for k in range(4):
        for x in range(4):
            at = (k * 4 + x) * PIECE
            out_ref[0, at : at + PIECE, :] = routed_ref[k, x, 0:24, :]
            out_ref[0, KEYS + at : KEYS + at + PIECE, :] = routed_ref[k, x, 24:48, :]
    rows = []
    for k in range(4):
        ids = sum(routed_ref[k, x, 48:56, :].astype(F32) for x in range(4))
        rows += [ids[0:1], ids[0:1], ids[1:2], ids[1:2]]
    out_ref[0, 2 * KEYS : ROWS, :] = jnp.concatenate(rows, axis=0).astype(BF16)


def reorder(source, out_ref, first):
    for e in range(2):
        for h in range(HEADS):
            at = first + h * SPAN
            out_ref[e, at : at + SPAN, :] = source[
                e * SPAN : (e + 1) * SPAN, h * HEAD_DIM : (h + 1) * HEAD_DIM
            ]


def reorder_kernel(source_ref, out_ref):
    reorder(source_ref, out_ref, 0)


def stack_kernel(own_ref, beyond_ref, ids_ref, out_ref):
    ids = id_rows(ids_ref, 16)
    reorder(beyond_ref, out_ref, COLS // 2)
    for e in range(2):
        out_ref[e, 0 : COLS // 2, :] = own_ref[e]
        out_ref[e, COLS : COLS + 16, :] = ids


def attend_kernel(mine, sets, start, width, has_state, last, *refs):
    refs = list(refs)
    q_refs = [refs.pop(0) for _ in sets]
    count = len(mine)
    block = [refs.pop(0) for _ in mine]
    state_ref = refs.pop(0) if has_state else None
    out_ref, turned, masks, one_hot, *held = refs
    weights, held = held[2:], held[:2]
    keys = KEYS * count

    turned[128:144, :] = jnp.ones((16, keys), BF16)
    for b in range(count):
        turned[0:128, b * KEYS : (b + 1) * KEYS] = block[b][0, KEYS : 2 * KEYS, :].T
    spot = lax.broadcasted_iota(jnp.int32, (SPAN, HEAD_DIM), 0)
    mark = lax.broadcasted_iota(jnp.int32, (SPAN, HEAD_DIM), 1)
    spike = jnp.where(spot == mark, 1.0, 0.0).astype(BF16)
    for k in range(2 * HEADS):
        one_hot[k * SPAN : (k + 1) * SPAN, :] = spike

    lane = lax.broadcasted_iota(jnp.int32, (PIECE, HEAD_DIM), 1)
    row = lax.broadcasted_iota(jnp.int32, (PIECE, HEAD_DIM), 0)
    ahead = (row - lane).astype(F32)
    core = lax.axis_index("core")

    def mask(s):
        query_row = q_refs[s // 2][s % 2, COLS : COLS + 16, :].astype(F32)[s % 2 : s % 2 + 1]
        for b in range(count):
            begin = ahead + ((core if mine[b] else 1 - core) * PIECE).astype(F32)
            places = block[b][0, 2 * KEYS : ROWS, :].astype(F32)
            limits = (query_row - places) * float(SPAN)
            for i in range(0, 16, 2):
                pieces = [
                    jnp.where(
                        begin + float(j % 2 * 2 * PIECE)
                        > jnp.broadcast_to(limits[j : j + 1], ahead.shape),
                        MASKED,
                        0.0,
                    )
                    for j in (i, i + 1)
                ]
                at = b * KEYS + i * PIECE
                masks[s, at : at + 2 * PIECE, :] = jnp.concatenate(pieces, axis=0).astype(BF16)

    flip = (((1,), (1,)), ((), ()))
    spans = 2 * len(sets)
    taken = slice(start, start + width)

    def score(s):
        mask(s)
        right = jnp.concatenate([q_refs[s // 2][s % 2, taken, :], one_hot[taken, :]], axis=1)
        best = None
        for b in range(count):
            rows = slice(b * KEYS, (b + 1) * KEYS)
            left = jnp.concatenate([block[b][0, 0:KEYS, :], masks[s, rows, :]], axis=1)
            part = lax.dot_general(left, right, flip, preferred_element_type=F32)
            held[s % 2][rows, :] = part
            peak = jnp.max(part.reshape(KEYS // (8 * GROUP), 8 * GROUP, width), axis=0)
            best = peak if best is None else jnp.maximum(best, peak)
        return best

    best = score(0)
    for s in range(spans):
        top = jnp.max(best, axis=0, keepdims=True)
        at = 2 * sets[0] + s
        if has_state:
            before = state_ref[at, 136:137, taken]
            top = jnp.maximum(before, top)
        for b in range(count):
            rows = slice(b * KEYS, (b + 1) * KEYS)
            weights[s % 2][rows, :] = jnp.exp2((held[s % 2][rows, :] - top) * FACTOR).astype(BF16)
        if s + 1 < spans:
            best = score(s + 1)
        for first in range(0, width, PART):
            inner = slice(first, min(first + PART, width))
            outer = slice(start + inner.start, start + inner.stop)
            sums = jnp.dot(turned[...], weights[s % 2][:, inner], preferred_element_type=F32)[0:136]
            peak = top[:, inner]
            if has_state:
                shrink = jnp.exp2((before[:, inner] - peak) * FACTOR)
                sums = sums + state_ref[at, 0:136, outer] * shrink
            if last:
                pack_state(out_ref, (s,), inner, sums[0:128], sums[128:129], peak)
            else:
                out_ref[s, 0:136, inner] = sums
                out_ref[s, 136:144, inner] = jnp.broadcast_to(peak, (8, peak.shape[1]))


def pack_state(out_ref, lead, cols, weighted, total, top):
    out_ref[(*lead, slice(0, 128), cols)] = weighted.astype(BF16)
    width = top.shape[1]
    line = lax.broadcasted_iota(jnp.int32, (16, width), 0)
    stats = jnp.zeros((16, width), F32)
    for base, value in ((0, top), (3, total)):
        for k in range(3):
            part = value.astype(BF16).astype(F32)
            value = value - part
            stats = jnp.where(line == base + k, jnp.broadcast_to(part, stats.shape), stats)
    out_ref[(*lead, slice(128, 144), cols)] = stats.astype(BF16)


def open_state(ref, lead, cols):
    stats = ref[(*lead, slice(128, 144), cols)].astype(F32)
    top = stats[0:1] + stats[1:2] + stats[2:3]
    total = stats[3:4] + stats[4:5] + stats[5:6]
    return ref[(*lead, slice(0, 128), cols)].astype(F32), total, top


def merge(mine, other):
    top = jnp.maximum(mine[2], other[2])
    a = jnp.exp2((mine[2] - top) * FACTOR)
    b = jnp.exp2((other[2] - top) * FACTOR)
    return mine[0] * a + other[0] * b, mine[1] * a + other[1] * b, top


def read_state(ref, e):
    return ref[e, 0:128, :], ref[e, 128:129, :], ref[e, 136:137, :]


def join_kernel(mine_ref, come_ref, out_ref):
    every = slice(0, COLS // 2)
    for e in range(2):
        merged = merge(read_state(mine_ref, e), open_state(come_ref, (e,), every))
        pack_state(out_ref, (e,), every, *merged)


def finish_kernel(mine_ref, core_ref, plane_ref, out_ref):
    every = slice(0, COLS // 2)
    for e in range(2):
        merged = merge(read_state(mine_ref, e), open_state(core_ref, (e,), every))
        weighted, total, _ = merge(merged, open_state(plane_ref, (e,), every))
        mixed = (weighted / total).T.astype(BF16)
        for h in range(HEADS):
            out_ref[e * SPAN : (e + 1) * SPAN, h * HEAD_DIM : (h + 1) * HEAD_DIM] = mixed[
                h * SPAN : (h + 1) * SPAN
            ]


def attend(stacks, sets, blocks, mine, state, last, start=0, width=COLS):
    count = len(blocks)
    steps = 2 * len(sets)
    keys = KEYS * count
    kernel = functools.partial(
        attend_kernel, mine, sets, start, width, state is not None, last
    )
    args = [stacks[s] for s in sets] + list(blocks)
    if state is not None:
        args.append(state)
    macs = steps * width * keys * (256 + STATE)
    return pl.pallas_call(
        kernel,
        out_shape=jax.ShapeDtypeStruct((steps, STATE, width), BF16 if last else F32),
        scratch_shapes=[
            pltpu.VMEM((STATE, keys), BF16),
            pltpu.VMEM((steps, keys, HEAD_DIM), BF16),
            pltpu.VMEM((COLS, HEAD_DIM), BF16),
            pltpu.VMEM((keys, width), F32),
            pltpu.VMEM((keys, width), F32),
            pltpu.VMEM((keys, width), BF16),
            pltpu.VMEM((keys, width), BF16),
        ],
        compiler_params=pltpu.CompilerParams(vmem_limit_bytes=14 * 1024 * 1024),
        cost_estimate=pl.CostEstimate(
            flops=4 * macs, bytes_accessed=2**20, transcendentals=steps * width * keys
        ),
    )(*args)


def call(kernel, out_shape, *args):
    spaces = [pltpu.SMEM if arg.dtype == jnp.int32 else pltpu.VMEM for arg in args]
    return pl.pallas_call(
        kernel,
        in_specs=[pl.BlockSpec(memory_space=space) for space in spaces],
        out_shape=out_shape,
        compiler_params=pltpu.CompilerParams(vmem_limit_bytes=8 * 1024 * 1024),
        cost_estimate=pl.CostEstimate(flops=2**21, bytes_accessed=2**20, transcendentals=0),
    )(*args)


def around(value):
    zs = lax.axis_size("z")
    perm = []
    for z in range(zs):
        perm.append((2 * z, 2 * ((z - 1) % zs)))
        perm.append((2 * z + 1, 2 * ((z + 1) % zs) + 1))
    return lax.ppermute(value, ("z", "core"), perm)


def shifted(value, axis, step):
    size = lax.axis_size(axis)
    return lax.ppermute(value, axis, [(i, (i + step) % size) for i in range(size)])


def ids_to_keys(ids):
    size = {a: lax.axis_size(a) for a in AXES}

    def flat(g, z, x, core):
        return ((g * size["z"] + z) * size["x"] + x) * size["core"] + core

    perm = []
    for g in range(8):
        for z in range(8):
            for core in range(2):
                perm.append((flat(g ^ core, g, z // 2, z % 2), flat(g, z, z // 2, core)))
    return lax.ppermute(ids, AXES, perm)


def body(query_rows, key_rows, value_rows, span_ids):
    places = ids_to_keys(span_ids)
    packed = call(
        pack_kernel,
        jax.ShapeDtypeStruct((4, 4, 56, HEAD_DIM), BF16),
        key_rows,
        value_rows,
        places,
    ).reshape(16, 56, HEAD_DIM)
    routed = lax.all_to_all(packed, ("kv", "x"), 0, 0, tiled=True)
    routed = routed.reshape(4, 4, 56, HEAD_DIM)
    near = call(spread_kernel, jax.ShapeDtypeStruct((1, ROWS, HEAD_DIM), BF16), routed)
    beyond = shifted(query_rows, "pair", 1)
    own = call(
        reorder_kernel, jax.ShapeDtypeStruct((2, COLS // 2, HEAD_DIM), BF16), query_rows
    )
    stack = call(
        stack_kernel,
        jax.ShapeDtypeStruct((2, COLS + 16, HEAD_DIM), BF16),
        own,
        beyond,
        span_ids,
    )
    stacks = (stack, shifted(stack, "core", 1))
    own_line, other_line = [], []
    own_line.append(around(near))
    mate = shifted(near, "core", 1)
    other_line.append(around(mate))
    for k in range(1, 4):
        own_line.append(around(own_line[-1]))
        if k < 3:
            other_line.append(around(other_line[-1]))
    state = None
    parts = [
        ([near, own_line[0]], [True, True]),
        ([other_line[0], own_line[1]], [False, True]),
        ([other_line[1], own_line[2]], [False, True]),
        ([other_line[2]], [False]),
    ]
    for blocks, mine in parts:
        state = attend(stacks, (0, 1), blocks, mine, state, False)
    far = own_line[3]
    half = COLS // 2
    packed_half = jax.ShapeDtypeStruct((2, STATE, half), BF16)
    leaving = attend(stacks, (1,), [far], [True], state, True, half, half)
    coming = shifted(leaving, "core", 1)
    mine = attend(stacks, (0,), [far], [True], state, False, half, half)
    joined = call(join_kernel, packed_half, mine, coming)
    plane = shifted(joined, "pair", 1)
    leaving = attend(stacks, (1,), [far], [True], state, True, 0, half)
    coming = shifted(leaving, "core", 1)
    mine = attend(stacks, (0,), [far], [True], state, False, 0, half)
    return call(
        finish_kernel,
        jax.ShapeDtypeStruct((2 * SPAN, HEADS * HEAD_DIM), BF16),
        mine,
        coming,
        plane,
    )


def solution(mesh):
    split = Mesh(mesh.devices.reshape(4, 2, 8, 4, 2), AXES)
    groups = ("kv", "pair")
    return jax.shard_map(
        body,
        mesh=split,
        in_specs=(P(BLK, groups), P(groups + BLK, None), P(groups + BLK, None), P(BLK)),
        out_specs=P(BLK, groups),
        check_vma=False,
    )
```
